256 devices in a mesh: ta: 32 (over z, x_hi, core), gz: 2 (over x_lo), gy: 4 (over y).
Axes of the slice: x: 4 (x_hi: 2, x_lo: 2; x = x_hi * 2 + x_lo), y: 4, z: 8, core: 2. Of those that a mesh axis runs over, the one named last changes fastest.
Arguments:
- lattice_links: float32 [2, 4, 18, 64, 16, 1024], P(None, None, None, 'ta', 'gz', 'gy'), may hold values from -1 to 1, as said below
- transform: float32 [2, 18, 64, 16, 1024], P(None, None, 'ta', 'gz', 'gy'), may hold values from -1 to 1, as said below
Outputs:
- fixed_transform: float32 [2, 18, 64, 16, 1024], P(None, None, 'ta', 'gz', 'gy')
- monitor: float32 [2, 2], replicated
The draws below stay inside these ranges and needn't reach their ends.
Inputs may be any that keep to these rules, and one draw needn't show every extreme that they name: `lattice_links`: every site's matrix for every colour and direction is special unitary. `transform`: every site's matrix is special unitary.
All inputs are finite; a program needn't handle non-finite values.
Results may differ from the reference program's by a relative error of at most 0.0003.
Values sent between devices are 32-bit elements; how exact they have to be, the bound alone decides.
No kernel may reach another device: no remote copies, remote signals or barrier semaphores. Data moves between devices by JAX's collectives and lax.ppermute only.
A program may use at most 128 MiB of HBM per device.

```python
import math
import jax
import jax.numpy as jnp

NX = 64
ITERS = 2
NT = 64
NZ = 16
NY = 32


def turn_rows(mat_re, mat_im, quat, row_one, row_two):
    q_zero, q_one, q_two, q_three = quat
    upper_re, upper_im = (mat_re[row_one], mat_im[row_one])
    lower_re, lower_im = (mat_re[row_two], mat_im[row_two])
    top_re = q_zero * upper_re - q_three * upper_im + q_two * lower_re - q_one * lower_im
    top_im = q_zero * upper_im + q_three * upper_re + q_two * lower_im + q_one * lower_re
    bottom_re = -q_two * upper_re - q_one * upper_im + q_zero * lower_re + q_three * lower_im
    bottom_im = -q_two * upper_im + q_one * upper_re + q_zero * lower_im - q_three * lower_re
    rows_re = [mat_re[0], mat_re[1], mat_re[2]]
    rows_im = [mat_im[0], mat_im[1], mat_im[2]]
    rows_re[row_one] = top_re
    rows_im[row_one] = top_im
    rows_re[row_two] = bottom_re
    rows_im[row_two] = bottom_im
    return (jnp.stack(rows_re, 0), jnp.stack(rows_im, 0))


def special_unitary(key, lead, spread):
    ones = (1,) * len(lead)
    identity = jnp.eye(3, dtype=jnp.float32).reshape((3, 3) + ones)
    mat_re = identity + jnp.zeros((3, 3) + lead, jnp.float32)
    mat_im = jnp.zeros((3, 3) + lead, jnp.float32)
    pairs = ((0, 1), (0, 2), (1, 2), (0, 1), (0, 2), (1, 2))
    for number in range(6):
        keys = jax.random.split(jax.random.fold_in(key, number), 3)
        spread_angle = spread * jax.random.normal(keys[0], lead, jnp.float32)
        phase_one = math.pi * jax.random.uniform(keys[1], lead, jnp.float32, -1.0, 1.0)
        phase_two = math.pi * jax.random.uniform(keys[2], lead, jnp.float32, -1.0, 1.0)
        cos_a = jnp.cos(spread_angle)
        sin_a = jnp.sin(spread_angle)
        quat = (cos_a * jnp.cos(phase_one), cos_a * jnp.sin(phase_one), sin_a * jnp.cos(phase_two), sin_a * jnp.sin(phase_two))
        row_one, row_two = pairs[number]
        mat_re, mat_im = turn_rows(mat_re, mat_im, quat, row_one, row_two)
    return (mat_re, mat_im)


def draw_lattice_links(key, part):
    row_len = NY * NX // 2
    times = jnp.arange(NT, dtype=jnp.float32).reshape((1, 1, NT, 1, 1)) / NT
    spread = 0.4 + 0.8 * times
    mat_re, mat_im = special_unitary(jax.random.fold_in(key, 17), (2, 4, NT, NZ, row_len), spread)
    stacked = jnp.stack([mat_re, mat_im], 0)
    stacked = jnp.transpose(stacked, (3, 4, 0, 1, 2, 5, 6, 7))
    return stacked.reshape((2, 4, 18, NT, NZ, row_len)).astype(jnp.float32)


def draw_transform(key, part):
    row_len = NY * NX // 2
    times = jnp.arange(NT, dtype=jnp.float32).reshape((1, NT, 1, 1)) / NT
    spread = 0.3 + 0.9 * times
    mat_re, mat_im = special_unitary(jax.random.fold_in(key, 29), (2, NT, NZ, row_len), spread)
    stacked = jnp.stack([mat_re, mat_im], 0)
    stacked = jnp.transpose(stacked, (3, 0, 1, 2, 4, 5, 6))
    return stacked.reshape((2, 18, NT, NZ, row_len)).astype(jnp.float32)


def setup_inputs(seed: int = 0) -> dict:
    key_list = jax.random.split(jax.random.key(seed), 3)
    return {
        "lattice_links": draw_lattice_links(jax.random.fold_in(key_list[2], 71), 0),
        "transform": draw_transform(jax.random.fold_in(key_list[2], 71), 0),
    }


OMEGA = 1.7
GUARD = 1e-12

def split_matrix(values):
    lead = values.shape[1:]
    return (values[:9].reshape((3, 3) + lead), values[9:].reshape((3, 3) + lead))

def join_matrix(mat_re, mat_im):
    lead = mat_re.shape[2:]
    return jnp.concatenate([mat_re.reshape((9,) + lead), mat_im.reshape((9,) + lead)], 0)

def product(left_re, left_im, right_re, right_im):
    total_re = None
    total_im = None
    for inner in range(3):
        col_re = left_re[:, inner][:, None]
        col_im = left_im[:, inner][:, None]
        row_re = right_re[inner][None]
        row_im = right_im[inner][None]
        term_re = col_re * row_re - col_im * row_im
        term_im = col_re * row_im + col_im * row_re
        if total_re is None:
            total_re = term_re
            total_im = term_im
        else:
            total_re = total_re + term_re
            total_im = total_im + term_im
    return (total_re, total_im)

def adjoint(mat_re, mat_im):
    return (jnp.swapaxes(mat_re, 0, 1), -jnp.swapaxes(mat_im, 0, 1))

def along_x(values, offset, forward, half_len):
    column = jnp.arange(values.shape[-1], dtype=jnp.int32) % half_len
    if forward:
        stepped = jnp.where(column == half_len - 1, jnp.roll(values, half_len - 1, -1), jnp.roll(values, -1, -1))
        return jnp.where(offset == 0, values, stepped)
    stepped = jnp.where(column == 0, jnp.roll(values, 1 - half_len, -1), jnp.roll(values, 1, -1))
    return jnp.where(offset == 0, stepped, values)

def rotation(mat_re, mat_im, row_one, row_two):
    vec_zero = mat_re[row_one, row_one] + mat_re[row_two, row_two]
    vec_one = -(mat_im[row_one, row_two] + mat_im[row_two, row_one])
    vec_two = mat_re[row_two, row_one] - mat_re[row_one, row_two]
    vec_three = -(mat_im[row_one, row_one] - mat_im[row_two, row_two])
    length = jnp.sqrt(vec_zero * vec_zero + vec_one * vec_one + vec_two * vec_two + vec_three * vec_three)
    step_zero = (1.0 - OMEGA) * length + OMEGA * vec_zero
    step_one = OMEGA * vec_one
    step_two = OMEGA * vec_two
    step_three = OMEGA * vec_three
    divisor = jnp.sqrt(step_zero * step_zero + step_one * step_one + step_two * step_two + step_three * step_three + GUARD)
    return (step_zero / divisor, step_one / divisor, step_two / divisor, step_three / divisor)

def rotate(mat_re, mat_im, quat, row_one, row_two):
    q_zero, q_one, q_two, q_three = quat
    upper_re, upper_im = (mat_re[row_one], mat_im[row_one])
    lower_re, lower_im = (mat_re[row_two], mat_im[row_two])

    def combine(left_pair, right_pair):
        left_re, left_im = (left_pair[0][None], left_pair[1][None])
        right_re, right_im = (right_pair[0][None], right_pair[1][None])
        new_re = left_re * upper_re - left_im * upper_im + right_re * lower_re - right_im * lower_im
        new_im = left_re * upper_im + left_im * upper_re + right_re * lower_im + right_im * lower_re
        return (new_re, new_im)
    top_re, top_im = combine((q_zero, q_three), (q_two, q_one))
    bottom_re, bottom_im = combine((-q_two, q_one), (q_zero, -q_three))
    rows_re = [mat_re[0], mat_re[1], mat_re[2]]
    rows_im = [mat_im[0], mat_im[1], mat_im[2]]
    rows_re[row_one] = top_re
    rows_im[row_one] = top_im
    rows_re[row_two] = bottom_re
    rows_im[row_two] = bottom_im
    return (jnp.stack(rows_re, 0), jnp.stack(rows_im, 0))

def relax(own, own_links, forward, backward):
    gauge_re, gauge_im = split_matrix(own)
    sum_re = None
    sum_im = None
    for direction in range(4):
        link_re, link_im = split_matrix(own_links[direction])
        next_re, next_im = adjoint(forward[direction][0], forward[direction][1])
        ahead_re, ahead_im = product(link_re, link_im, next_re, next_im)
        behind_re, behind_im = adjoint(backward[direction][0], backward[direction][1])
        if sum_re is None:
            sum_re = ahead_re + behind_re
            sum_im = ahead_im + behind_im
        else:
            sum_re = sum_re + ahead_re + behind_re
            sum_im = sum_im + ahead_im + behind_im
    mat_re, mat_im = product(gauge_re, gauge_im, sum_re, sum_im)
    for row_one, row_two in ((0, 1), (0, 2), (1, 2)):
        quat = rotation(mat_re, mat_im, row_one, row_two)
        mat_re, mat_im = rotate(mat_re, mat_im, quat, row_one, row_two)
        gauge_re, gauge_im = rotate(gauge_re, gauge_im, quat, row_one, row_two)
    return (join_matrix(gauge_re, gauge_im), mat_re, mat_im)

def measures(mat_re, mat_im):
    diag_sum = mat_re[0, 0] + mat_re[1, 1] + mat_re[2, 2]
    skew_re = 0.5 * (mat_re - jnp.swapaxes(mat_re, 0, 1))
    skew_im = 0.5 * (mat_im + jnp.swapaxes(mat_im, 0, 1))
    mean_im = (skew_im[0, 0] + skew_im[1, 1] + skew_im[2, 2]) / 3.0
    identity = jnp.eye(3, dtype=jnp.float32).reshape((3, 3) + (1,) * diag_sum.ndim)
    skew_im = skew_im - identity * mean_im[None, None]
    return (jnp.sum(diag_sum), jnp.sum(skew_re * skew_re + skew_im * skew_im))

def neighbour(values, direction, sign, offset, half_len):
    if direction == 0:
        return along_x(values, offset, sign > 0, half_len)
    if direction == 1:
        return jnp.roll(values, -sign * half_len, -1)
    if direction == 2:
        return jnp.roll(values, -sign, -2)
    return jnp.roll(values, -sign, -3)

def reference(lattice_links, transform):
    half_len = NX // 2
    row_len = lattice_links.shape[-1]
    t_index = jnp.arange(NT, dtype=jnp.int32)[:, None, None]
    z_index = jnp.arange(NZ, dtype=jnp.int32)[None, :, None]
    y_index = (jnp.arange(row_len, dtype=jnp.int32) // half_len)[None, None, :]
    parity = t_index + z_index + y_index
    offsets = [parity % 2, (parity + 1) % 2]
    colours = [transform[0], transform[1]]
    func_list = []
    div_list = []
    for sweep in range(ITERS):
        for colour in (0, 1):
            partner = 1 - colour
            offset = offsets[colour]
            part_re, part_im = split_matrix(colours[partner])
            forward = []
            backward = []
            for direction in range(4):
                forward.append((neighbour(part_re, direction, 1, offset, half_len), neighbour(part_im, direction, 1, offset, half_len)))
                link_re, link_im = split_matrix(lattice_links[partner, direction])
                prod_re, prod_im = product(part_re, part_im, link_re, link_im)
                backward.append((neighbour(prod_re, direction, -1, offset, half_len), neighbour(prod_im, direction, -1, offset, half_len)))
            colours[colour], mat_re, mat_im = relax(colours[colour], lattice_links[colour], forward, backward)
        func_sum, div_sum = measures(mat_re, mat_im)
        func_list.append(func_sum)
        div_list.append(div_sum)
    volume = NT * NZ * NY * NX
    sums = jnp.stack([jnp.stack(func_list), jnp.stack(div_list)], 0)
    monitor = jnp.stack([1.0 - sums[0] / (12.0 * volume), sums[1] / (volume / 2.0)], 0)
    return (jnp.stack(colours, 0), monitor)
```

```python
import functools

import jax
import jax.numpy as jnp
from jax import lax
from jax.experimental import pallas as pl
from jax.experimental.pallas import tpu as pltpu
from jax.sharding import Mesh
from jax.sharding import PartitionSpec as P

NX = 64
ITERS = 2
OMEGA = 1.7
GUARD = 1e-12
TA = ("tz", "tx", "tc")
F32 = jnp.float32
R3 = range(3)


def re(i, j):
    return 3 * i + j


def im(i, j):
    return 9 + 3 * i + j


def half(h):
    return pl.ds(128 * h, 128)


def times_adjoint(acc, left, right):
    out = list(acc)
    for k in R3:
        lr = [left(re(i, k)) for i in R3]
        li = [left(im(i, k)) for i in R3]
        rr = [right(re(j, k)) for j in R3]
        ri = [right(im(j, k)) for j in R3]
        for i in R3:
            for j in R3:
                tr = lr[i] * rr[j] + li[i] * ri[j]
                ti = li[i] * rr[j] - lr[i] * ri[j]
                a, b = re(i, j), im(i, j)
                out[a] = tr if out[a] is None else out[a] + tr
                out[b] = ti if out[b] is None else out[b] + ti
    return out


def times(left, right):
    out = [None] * 18
    for k in R3:
        lr = [left(re(i, k)) for i in R3]
        li = [left(im(i, k)) for i in R3]
        rr = [right(re(k, j)) for j in R3]
        ri = [right(im(k, j)) for j in R3]
        for i in R3:
            for j in R3:
                tr = lr[i] * rr[j] - li[i] * ri[j]
                ti = lr[i] * ri[j] + li[i] * rr[j]
                a, b = re(i, j), im(i, j)
                out[a] = tr if out[a] is None else out[a] + tr
                out[b] = ti if out[b] is None else out[b] + ti
    return out


def plus_adjoint(acc, mat):
    out = list(acc)
    for i in R3:
        for j in R3:
            out[re(i, j)] = out[re(i, j)] + mat[re(j, i)]
            out[im(i, j)] = out[im(i, j)] - mat[im(j, i)]
    return out


def rotation(a, p, q):
    v0 = a[re(p, p)] + a[re(q, q)]
    v1 = -(a[im(p, q)] + a[im(q, p)])
    v2 = a[re(q, p)] - a[re(p, q)]
    v3 = -(a[im(p, p)] - a[im(q, q)])
    length = jnp.sqrt(v0 * v0 + v1 * v1 + v2 * v2 + v3 * v3)
    s0 = (1.0 - OMEGA) * length + OMEGA * v0
    s1, s2, s3 = OMEGA * v1, OMEGA * v2, OMEGA * v3
    inverse = lax.rsqrt(s0 * s0 + s1 * s1 + s2 * s2 + s3 * s3 + GUARD)
    return s0 * inverse, s1 * inverse, s2 * inverse, s3 * inverse


def rotate(m, quat, p, q):
    q0, q1, q2, q3 = quat
    out = list(m)
    for j in R3:
        ur, ui = m[re(p, j)], m[im(p, j)]
        lr, li = m[re(q, j)], m[im(q, j)]
        out[re(p, j)] = q0 * ur - q3 * ui + q2 * lr - q1 * li
        out[im(p, j)] = q0 * ui + q3 * ur + q2 * li + q1 * lr
        out[re(q, j)] = q0 * lr + q3 * li - q2 * ur - q1 * ui
        out[im(q, j)] = q0 * li - q3 * lr - q2 * ui + q1 * ur
    return out


def relax(g, w):
    a = times(lambda c: g[c], lambda c: w[c])
    for p, q in ((0, 1), (0, 2), (1, 2)):
        quat = rotation(a, p, q)
        a = rotate(a, quat, p, q)
        g = rotate(g, quat, p, q)
    return g, a


def measures(a):
    func = a[re(0, 0)] + a[re(1, 1)] + a[re(2, 2)]
    off = None
    for i, j in ((0, 1), (0, 2), (1, 2)):
        dr = a[re(i, j)] - a[re(j, i)]
        di = a[im(i, j)] + a[im(j, i)]
        term = dr * dr + di * di
        off = term if off is None else off + term
    mean = (a[im(0, 0)] + a[im(1, 1)] + a[im(2, 2)]) / 3.0
    div = 0.5 * off
    for i in R3:
        d = a[im(i, i)] - mean
        div = div + d * d
    return func, div


def unit(c):
    return 1.0 if c in (0, 4, 8) else 0.0


def crossing(links, h, is_unit):
    return lambda c: jnp.where(is_unit, F32(unit(c)), links[3, c, 1, :, half(h)])


def iotas():
    return (
        lax.broadcasted_iota(jnp.int32, (8, 128), 0),
        lax.broadcasted_iota(jnp.int32, (8, 128), 1),
    )


def pack_links(links, upz, upy):
    row, lane = iotas()
    for c in range(18):
        upz[c] = jnp.full((8, 128), unit(c), F32)
        for t in range(2):
            for h in range(2):
                r = 4 + 2 * t + h
                upz[c, r : r + 1, :] = links[2, c, t, 7:8, half(h)]
        high0 = pltpu.roll(links[1, c, 0, :, half(1)], 96, 1)
        high1 = links[1, c, 1, :, half(1)]
        upy[c] = jnp.where(lane < 64, F32(unit(c)), jnp.where(lane < 96, high0, high1))


def pack_sides(g, upz, upy, zp, yp, scr):
    row, lane = iotas()
    for c in range(18):
        for t in range(2):
            for h in range(2):
                r = 2 * t + h
                scr[c, r : r + 1, :] = g[c, t, 0:1, half(h)]
                scr[c, 4 + r : 5 + r, :] = g[c, t, 7:8, half(h)]
    out = times(lambda c: scr[c], lambda c: upz[c])
    for c in range(18):
        zp[c] = out[c]
    side = []
    for c in range(18):
        low1 = pltpu.roll(g[c, 1, :, half(0)], 32, 1)
        high0 = pltpu.roll(g[c, 0, :, half(1)], 96, 1)
        side.append(
            jnp.where(
                lane < 64,
                jnp.where(lane < 32, g[c, 0, :, half(0)], low1),
                jnp.where(lane < 96, high0, g[c, 1, :, half(1)]),
            )
        )
    out = times(lambda c: side[c], lambda c: upy[c])
    for c in range(18):
        yp[c] = out[c]


def first_kernel(links0, links1, g, tp, fp, zp, yp, upz0, upy0, upz1, upy1, scr):
    core = lax.axis_index("tc")
    pack_links(links1, upz1, upy1)
    for h in range(2):
        for out, s, is_unit in ((fp, core, core == 0), (tp, 1 - core, core == 1)):
            face = times(lambda c: g[c, s, :, half(h)], crossing(links1, h, is_unit))
            for c in range(18):
                out[c, :, half(h)] = face[c]
    pack_sides(g, upz1, upy1, zp, yp, scr)
    pack_links(links0, upz0, upy0)


def near_kernel(colour, last, own, other, gp, g, zh, ya, yb, th, *refs):
    if last:
        gn, wf, sums, w_scr, y_scr = refs
    else:
        gn, wf, tp, sums, w_scr, y_scr = refs
    core = lax.axis_index("tc")
    odd_row = lax.axis_index("gy") % 2
    row, lane = iotas()
    column = lane % 32
    parity = (row + lane // 32) % 2
    from_a = (lane // 64) == odd_row
    for c in range(18):
        y_scr[c] = jnp.where(from_a, ya[c], yb[c])
    for s in range(2):
        stays = parity == (s + colour) % 2
        behind = []
        for h in range(2):
            behind.append(
                times(lambda c: gp[c, s, :, half(h)], lambda c: other[1, c, s, :, half(h)])
            )
        low, high = [], []
        for c in range(18):
            r0 = pltpu.roll(behind[0][c], 32, 1)
            r1 = pltpu.roll(behind[1][c], 32, 1)
            halo = pltpu.roll(y_scr[c], 64 - 32 * s, 1)
            low.append(jnp.where(lane < 32, halo, r0))
            high.append(jnp.where(lane < 32, r0, r1))
        for h, mat in ((0, low), (1, high)):
            zero = [jnp.zeros((8, 128), F32)] * 18
            acc = plus_adjoint(zero, mat)
            for c in range(18):
                w_scr[c, s, :, half(h)] = acc[c]
        for h in range(2):
            acc = [w_scr[c, s, :, half(h)] for c in range(18)]

            def tile(c):
                return gp[c, s, :, half(h)]

            def ahead_x(c):
                v = tile(c)
                step = jnp.where(column == 31, pltpu.roll(v, 31, 1), pltpu.roll(v, 127, 1))
                return jnp.where(stays, v, step)

            acc = times_adjoint(acc, lambda c: own[0, c, s, :, half(h)], ahead_x)

            def ahead_y(c):
                a = pltpu.roll(gp[c, s, :, half(1)], 96, 1)
                if h == 0:
                    return jnp.where(lane >= 96, a, pltpu.roll(tile(c), 96, 1))
                return jnp.where(lane >= 96, pltpu.roll(y_scr[c], 96 - 32 * s, 1), a)

            acc = times_adjoint(acc, lambda c: own[1, c, s, :, half(h)], ahead_y)
            r = 2 * s + h

            def ahead_z(c):
                halo = jnp.broadcast_to(zh[c, r : r + 1, :], (8, 128))
                return jnp.where(row == 7, halo, pltpu.roll(tile(c), 7, 0))

            acc = times_adjoint(acc, lambda c: own[2, c, s, :, half(h)], ahead_z)
            back = times(tile, lambda c: other[0, c, s, :, half(h)])
            shifted = []
            for v in back:
                step = jnp.where(column == 0, pltpu.roll(v, 97, 1), pltpu.roll(v, 1, 1))
                shifted.append(jnp.where(stays, step, v))
            acc = plus_adjoint(acc, shifted)
            back = times(tile, lambda c: other[2, c, s, :, half(h)])
            shifted = []
            for c, v in enumerate(back):
                halo = jnp.broadcast_to(zh[c, 4 + r : 5 + r, :], (8, 128))
                shifted.append(jnp.where(row == 0, halo, pltpu.roll(v, 1, 0)))
            acc = plus_adjoint(acc, shifted)
            if s == 0:
                acc = times_adjoint(
                    acc,
                    lambda c: own[3, c, 0, :, half(h)],
                    lambda c: gp[c, 1, :, half(h)],
                )
            else:
                back = times(
                    lambda c: gp[c, 0, :, half(h)], lambda c: other[3, c, 0, :, half(h)]
                )
                acc = plus_adjoint(acc, back)
            for c in range(18):
                w_scr[c, s, :, half(h)] = acc[c]
    near = 1 - core
    total = [jnp.zeros((8, 128), F32)] * 2
    for h in range(2):
        for c in range(18):
            wf[c, :, half(h)] = w_scr[c, core, :, half(h)]
        link = crossing(own, h, core == 1)
        acc = [w_scr[c, near, :, half(h)] for c in range(18)]
        acc = times_adjoint(acc, link, lambda c: th[c, :, half(h)])
        new, mat = relax([g[c, near, :, half(h)] for c in range(18)], acc)
        for c in range(18):
            gn[c, :, half(h)] = new[c]
        if not last:
            face = times(lambda c: new[c], link)
            for c in range(18):
                tp[c, :, half(h)] = face[c]
        if colour == 1:
            total = [a + b for a, b in zip(total, measures(mat))]
    sums[0] = total[0]
    sums[1] = total[1]


def far_kernel(colour, last, own, g, gn, wf, fh, near_sums, *refs):
    if last:
        g0, out, sums = refs
    else:
        upz, upy, out, fp, zp, yp, sums, scr = refs
    core = lax.axis_index("tc")
    total = [near_sums[0], near_sums[1]]
    for h in range(2):
        link = crossing(own, h, core == 0)
        acc = [wf[c, :, half(h)] for c in range(18)]
        acc = times_adjoint(acc, link, lambda c: fh[c, :, half(h)])
        new, mat = relax([g[c, core, :, half(h)] for c in range(18)], acc)
        if last:
            for c in range(18):
                out[1, c, core, :, half(h)] = new[c]
        else:
            for c in range(18):
                out[c, core, :, half(h)] = new[c]
            face = times(lambda c: new[c], link)
            for c in range(18):
                fp[c, :, half(h)] = face[c]
        if colour == 1:
            total = [a + b for a, b in zip(total, measures(mat))]
    if last:
        for c in range(18):
            out[1, c, 1 - core] = gn[c]
            for s in range(2):
                out[0, c, s] = g0[c, s]
    else:
        for c in range(18):
            out[c, 1 - core] = gn[c]
        pack_sides(out, upz, upy, zp, yp, scr)
    if colour == 1:
        for k in range(2):
            rows = jnp.sum(total[k], axis=0, keepdims=True)
            sums[k] = jnp.broadcast_to(jnp.sum(rows, axis=1, keepdims=True), (8, 128))
    else:
        sums[0] = total[0]
        sums[1] = total[1]


def final_kernel(volume, parts, monitor):
    total = parts[0]
    for k in range(1, parts.shape[0]):
        total = total + parts[k]
    row, lane = iotas()
    func = jnp.where(lane[:4] == 0, total[0:1], total[2:3])
    div = jnp.where(lane[:4] == 0, total[1:2], total[3:4])
    both = jnp.where(row[:4] == 0, 1.0 - func / (12.0 * volume), div / (volume / 2.0))
    monitor[...] = both[:2, :2]


def call(body, outs, scratch, args, flops, name):
    return pl.pallas_call(
        body,
        out_shape=[jax.ShapeDtypeStruct(o, F32) for o in outs],
        in_specs=[pl.BlockSpec(memory_space=pltpu.VMEM)] * len(args),
        out_specs=[pl.BlockSpec(memory_space=pltpu.VMEM)] * len(outs),
        scratch_shapes=[pltpu.VMEM(s, F32) for s in scratch],
        compiler_params=pltpu.CompilerParams(vmem_limit_bytes=24 * 2**20),
        cost_estimate=pl.CostEstimate(flops=flops, bytes_accessed=0, transcendentals=0),
        name=name,
    )(*args)


def swap(value, axis, partner):
    count = lax.axis_size(axis)
    return lax.ppermute(value, axis, [(i, partner(i) % count) for i in range(count)])


def even_odd(i):
    return i ^ 1


def odd_even(i):
    return i + 1 if i % 2 else i - 1


def gathered(values, axes):
    count = 1
    for axis in axes:
        count *= lax.axis_size(axis)
    parts = jnp.broadcast_to(values, (count,) + values.shape)
    return lax.all_to_all(parts, axes, 0, 0, tiled=True)


FACE = (18, 8, 256)
SIDE = (18, 8, 128)
FIELD = (18, 2, 8, 256)


def shards(lattice_links, transform):
    links = [lattice_links[0], lattice_links[1]]
    g = [transform[0], transform[1]]
    packed = [None, None]
    tp, fp, zp, yp, *sides = call(
        first_kernel,
        [FACE, FACE, SIDE, SIDE] + [SIDE] * 4,
        [SIDE],
        [links[0], links[1], g[1]],
        10**7,
        "first",
    )
    packed[0] = sides[:2]
    packed[1] = sides[2:]
    volume = 2 * transform.shape[2] * transform.shape[3] * transform.shape[4]
    for axis in TA + ("gz", "gy"):
        volume *= lax.axis_size(axis)
    kept = []
    for sweep in range(ITERS):
        for colour in (0, 1):
            last = sweep == ITERS - 1 and colour == 1
            other = 1 - colour
            fh = swap(fp, TA, odd_even)
            zh = swap(zp, "gz", even_odd)
            ya = swap(yp, "gy", even_odd)
            yb = swap(yp, "gy", odd_even)
            th = swap(tp, "tc", even_odd)
            outs = [FACE, FACE] + ([] if last else [FACE]) + [(2, 8, 128)]
            gn, wf, *rest = call(
                functools.partial(near_kernel, colour, last),
                outs,
                [FIELD, SIDE],
                [links[colour], links[other], g[other], g[colour], zh, ya, yb, th],
                3 * 10**7,
                f"near_{sweep}_{colour}",
            )
            sums = rest[-1]
            args = [links[colour], g[colour], gn, wf, fh, sums]
            if last:
                out, sums = call(
                    functools.partial(far_kernel, colour, last),
                    [(2,) + FIELD, (2, 8, 128)],
                    [],
                    args + [g[0]],
                    10**7,
                    f"far_{sweep}_{colour}",
                )
            else:
                tp = rest[0]
                g[colour], fp, zp, yp, sums = call(
                    functools.partial(far_kernel, colour, last),
                    [FIELD, FACE, SIDE, SIDE, (2, 8, 128)],
                    [SIDE],
                    args + list(packed[colour]),
                    10**7,
                    f"far_{sweep}_{colour}",
                )
        kept.append(sums[:, 0, :])
    parts = gathered(jnp.concatenate(kept, 0), ("tx", "gz", "gy"))
    parts = gathered(jnp.sum(parts, 0), ("tz", "tc"))
    (monitor,) = call(
        functools.partial(final_kernel, volume), [(2, 2)], [], [parts], 10**3, "final"
    )
    return (out, monitor)


def solution(mesh):
    finer = Mesh(
        mesh.devices.reshape(8, 2, 2, mesh.shape["gz"], mesh.shape["gy"]),
        ("tz", "tx", "tc", "gz", "gy"),
    )
    return jax.shard_map(
        shards,
        mesh=finer,
        in_specs=(P(None, None, None, TA, "gz", "gy"), P(None, None, TA, "gz", "gy")),
        out_specs=(P(None, None, TA, "gz", "gy"), P()),
        check_vma=False,
    )
```

```python
import functools

import jax
import jax.numpy as jnp
from jax import lax
from jax.experimental import pallas as pl
from jax.experimental.pallas import tpu as pltpu
from jax.sharding import Mesh
from jax.sharding import PartitionSpec as P


ITERS = 2
OMEGA = 1.7
GUARD = 1e-12
TA = ("tz", "tx", "tc")
AXES = TA + ("gz", "gy")
F32 = jnp.float32
R3 = range(3)
PAIRS = ((0, 1), (0, 2), (1, 2))
ROWS = (0, 1, 2, 3, 4, 5, 9, 10, 11, 12, 13, 14)
TWO_ROWS, WHOLE, TURN = range(3)


def re(i, j):
    return 3 * i + j


def im(i, j):
    return 9 + 3 * i + j


def half(h):
    return pl.ds(128 * h, 128)


def times_adjoint(acc, left, right):
    out = list(acc)
    for k in R3:
        lr = [left(re(i, k)) for i in R3]
        li = [left(im(i, k)) for i in R3]
        rr = [right(re(j, k)) for j in R3]
        ri = [right(im(j, k)) for j in R3]
        for i in R3:
            for j in R3:
                tr = lr[i] * rr[j] + li[i] * ri[j]
                ti = li[i] * rr[j] - lr[i] * ri[j]
                a, b = re(i, j), im(i, j)
                out[a] = tr if out[a] is None else out[a] + tr
                out[b] = ti if out[b] is None else out[b] + ti
    return out


def times(left, right):
    out = [None] * 18
    for k in R3:
        lr = [left(re(i, k)) for i in R3]
        li = [left(im(i, k)) for i in R3]
        rr = [right(re(k, j)) for j in R3]
        ri = [right(im(k, j)) for j in R3]
        for i in R3:
            for j in R3:
                tr = lr[i] * rr[j] - li[i] * ri[j]
                ti = lr[i] * ri[j] + li[i] * rr[j]
                a, b = re(i, j), im(i, j)
                out[a] = tr if out[a] is None else out[a] + tr
                out[b] = ti if out[b] is None else out[b] + ti
    return out


def plus_adjoint(acc, mat):
    out = list(acc)
    for i in R3:
        for j in R3:
            out[re(i, j)] = out[re(i, j)] + mat[re(j, i)]
            out[im(i, j)] = out[im(i, j)] - mat[im(j, i)]
    return out


def rotation(a, p, q):
    v0 = a[re(p, p)] + a[re(q, q)]
    v1 = -(a[im(p, q)] + a[im(q, p)])
    v2 = a[re(q, p)] - a[re(p, q)]
    v3 = -(a[im(p, p)] - a[im(q, q)])
    length = jnp.sqrt(v0 * v0 + v1 * v1 + v2 * v2 + v3 * v3)
    s0 = (1.0 - OMEGA) * length + OMEGA * v0
    s1, s2, s3 = OMEGA * v1, OMEGA * v2, OMEGA * v3
    inverse = lax.rsqrt(s0 * s0 + s1 * s1 + s2 * s2 + s3 * s3 + GUARD)
    return s0 * inverse, s1 * inverse, s2 * inverse, s3 * inverse


def rotate(m, quat, p, q):
    q0, q1, q2, q3 = quat
    out = list(m)
    for j in R3:
        ur, ui = m[re(p, j)], m[im(p, j)]
        lr, li = m[re(q, j)], m[im(q, j)]
        out[re(p, j)] = q0 * ur - q3 * ui + q2 * lr - q1 * li
        out[im(p, j)] = q0 * ui + q3 * ur + q2 * li + q1 * lr
        out[re(q, j)] = q0 * lr + q3 * li - q2 * ur - q1 * ui
        out[im(q, j)] = q0 * li - q3 * lr - q2 * ui + q1 * ur
    return out


def relax(g, w):
    a = times(lambda c: g[c], lambda c: w[c])
    turn = []
    for p, q in PAIRS:
        quat = rotation(a, p, q)
        a = rotate(a, quat, p, q)
        g = rotate(g, quat, p, q)
        turn += quat
    return g, a, turn


def turned(mat, turn):
    for k, (p, q) in enumerate(PAIRS):
        mat = rotate(mat, turn[4 * k : 4 * k + 4], p, q)
    return mat


def third_row(rows):
    a = [None] * 18
    for c, v in zip(ROWS, rows):
        a[c] = v
    for j in R3:
        k, m = (j + 1) % 3, (j + 2) % 3
        ur, ui, xr, xi = a[re(0, k)], a[im(0, k)], a[re(1, m)], a[im(1, m)]
        vr, vi, yr, yi = a[re(0, m)], a[im(0, m)], a[re(1, k)], a[im(1, k)]
        a[re(2, j)] = (ur * xr - ui * xi) - (vr * yr - vi * yi)
        a[im(2, j)] = (vr * yi + vi * yr) - (ur * xi + ui * xr)
    return a


def behind(mode, sent, link, before):
    if mode == TURN:
        return turned([before[c] for c in range(18)], [sent(c) for c in range(12)])
    if mode == TWO_ROWS:
        full = third_row([sent(k) for k in range(12)])
        return times_adjoint([None] * 18, lambda c: full[c], link)
    return times_adjoint([None] * 18, sent, link)


def measures(a):
    func = a[re(0, 0)] + a[re(1, 1)] + a[re(2, 2)]
    off = None
    for i, j in PAIRS:
        dr = a[re(i, j)] - a[re(j, i)]
        di = a[im(i, j)] + a[im(j, i)]
        term = dr * dr + di * di
        off = term if off is None else off + term
    mean = (a[im(0, 0)] + a[im(1, 1)] + a[im(2, 2)]) / 3.0
    div = 0.5 * off
    for i in R3:
        d = a[im(i, i)] - mean
        div = div + d * d
    return func, div


def unit(c):
    return 1.0 if c in (0, 4, 8) else 0.0


def crossing(links, h, is_unit):
    return lambda c: jnp.where(is_unit, F32(unit(c)), links[3, c, 1, :, half(h)])


def iotas():
    return (
        lax.broadcasted_iota(jnp.int32, (8, 128), 0),
        lax.broadcasted_iota(jnp.int32, (8, 128), 1),
    )


def slices(core):
    return core, 1 - core


def pack_links(core, links, upz, upy):
    _, lane = iotas()
    for c in range(18):
        upz[c] = jnp.full((8, 128), unit(c), F32)
        for k, s in enumerate(slices(core)):
            for h in range(2):
                r = 4 + 2 * k + h
                upz[c, r : r + 1, :] = links[2, c, s, 7:8, half(h)]
        high0 = pltpu.roll(links[1, c, core, :, half(1)], 96, 1)
        high1 = links[1, c, 1 - core, :, half(1)]
        upy[c] = jnp.where(lane < 64, F32(unit(c)), jnp.where(lane < 96, high0, high1))


def pack_rows(c, k, value, h, scr):
    scr[c, 2 * k + h : 2 * k + h + 1, :] = value[0:1, :]
    scr[c, 4 + 2 * k + h : 5 + 2 * k + h, :] = value[7:8, :]


def pack_z(core, g, upz, zp, scr):
    for c in range(18):
        for k, s in enumerate(slices(core)):
            for h in range(2):
                pack_rows(c, k, g[c, s, :, half(h)], h, scr)
    out = times(lambda c: scr[c], lambda c: upz[c])
    for k, c in enumerate(ROWS if zp.shape[0] == 12 else range(18)):
        zp[k] = out[c]


def row_ends(value):
    _, lane = iotas()
    low1 = pltpu.roll(value(1, 0), 32, 1)
    high0 = pltpu.roll(value(0, 1), 96, 1)
    return jnp.where(
        lane < 64,
        jnp.where(lane < 32, value(0, 0), low1),
        jnp.where(lane < 96, high0, value(1, 1)),
    )


def send_rows(ends, lowp, highp):
    _, lane = iotas()
    for k in range(lowp.shape[0]):
        a, b = ends[2 * k], ends[2 * k + 1]
        lowp[k] = jnp.where(lane < 64, a, pltpu.roll(b, 64, 1))
        highp[k] = jnp.where(lane < 64, pltpu.roll(a, 64, 1), b)


def received_rows(c, yu, yd):
    _, lane = iotas()
    u, d = yu[c // 2], yd[c // 2]
    if c % 2:
        return jnp.where(lane < 64, pltpu.roll(u, 64, 1), d)
    return jnp.where(lane < 64, u, pltpu.roll(d, 64, 1))


def pack_y(core, g, upy, lowp, highp):
    ends = [
        row_ends(lambda k, h: g[c, slices(core)[k], :, half(h)]) for c in range(18)
    ]
    out = times(lambda c: ends[c], lambda c: upy[c])
    if lowp.shape[0] == 6:
        out = [out[c] for c in ROWS]
    send_rows(out, lowp, highp)


def first_kernel(
    links_hbm, g_hbm, links, g, tp, fp, zp, lowp, highp, upz0, upy0, upz1, upy1, scr, sems
):
    copies = []
    for colour in (1, 0):
        copies.append((g_hbm.at[colour], g.at[colour]))
        for mu in (3, 2, 1, 0):
            copies.append((links_hbm.at[colour, mu], links.at[colour, mu]))
    copies = [pltpu.make_async_copy(a, b, sems.at[k]) for k, (a, b) in enumerate(copies)]
    for copy in copies:
        copy.start()
    core = lax.axis_index("tc")
    far, near = slices(core)
    for copy in copies[:2]:
        copy.wait()
    for h in range(2):
        face = times(lambda c: g[1, c, far, :, half(h)], crossing(links.at[1], h, core == 0))
        for k, c in enumerate(ROWS):
            fp[k, :, half(h)] = face[c]
        face = times(lambda c: g[1, c, near, :, half(h)], crossing(links.at[1], h, core == 1))
        for c in range(18):
            tp[c, :, half(h)] = face[c]
    for copy in copies[2:4]:
        copy.wait()
    pack_links(core, links.at[1], upz1, upy1)
    pack_z(core, g.at[1], upz1, zp, scr)
    pack_y(core, g.at[1], upy1, lowp, highp)
    for copy in copies[4:]:
        copy.wait()
    pack_links(core, links.at[0], upz0, upy0)


def local_kernel(colour, first, links, gp, w):
    own, other = links.at[colour], links.at[1 - colour]
    if first:
        gp = gp.at[1 - colour]
    row, lane = iotas()
    column = lane % 32
    parity = (row + lane // 32) % 2
    for s in range(2):
        stays = parity == (s + colour) % 2
        behind = []
        for h in range(2):
            behind.append(
                times(lambda c: gp[c, s, :, half(h)], lambda c: other[1, c, s, :, half(h)])
            )
        low, high = [], []
        for c in range(18):
            r0 = pltpu.roll(behind[0][c], 32, 1)
            r1 = pltpu.roll(behind[1][c], 32, 1)
            low.append(jnp.where(lane < 32, 0.0, r0))
            high.append(jnp.where(lane < 32, r0, r1))
        for h, mat in ((0, low), (1, high)):
            acc = plus_adjoint([jnp.zeros((8, 128), F32)] * 18, mat)
            for c in range(18):
                w[c, s, :, half(h)] = acc[c]
        for h in range(2):
            acc = [w[c, s, :, half(h)] for c in range(18)]

            def tile(c):
                return gp[c, s, :, half(h)]

            def ahead_x(c):
                v = tile(c)
                step = jnp.where(column == 31, pltpu.roll(v, 31, 1), pltpu.roll(v, 127, 1))
                return jnp.where(stays, v, step)

            acc = times_adjoint(acc, lambda c: own[0, c, s, :, half(h)], ahead_x)

            def ahead_y(c):
                a = pltpu.roll(gp[c, s, :, half(1)], 96, 1)
                if h == 0:
                    return jnp.where(lane >= 96, a, pltpu.roll(tile(c), 96, 1))
                return jnp.where(lane >= 96, 0.0, a)

            acc = times_adjoint(acc, lambda c: own[1, c, s, :, half(h)], ahead_y)

            def ahead_z(c):
                return jnp.where(row == 7, 0.0, pltpu.roll(tile(c), 7, 0))

            acc = times_adjoint(acc, lambda c: own[2, c, s, :, half(h)], ahead_z)
            back = times(tile, lambda c: other[0, c, s, :, half(h)])
            shifted = []
            for v in back:
                step = jnp.where(column == 0, pltpu.roll(v, 97, 1), pltpu.roll(v, 1, 1))
                shifted.append(jnp.where(stays, step, v))
            acc = plus_adjoint(acc, shifted)
            back = times(tile, lambda c: other[2, c, s, :, half(h)])
            acc = plus_adjoint(acc, [jnp.where(row == 0, 0.0, pltpu.roll(v, 1, 0)) for v in back])
            if s == 0:
                acc = times_adjoint(
                    acc,
                    lambda c: own[3, c, 0, :, half(h)],
                    lambda c: gp[c, 1, :, half(h)],
                )
            else:
                back = times(
                    lambda c: gp[c, 0, :, half(h)], lambda c: other[3, c, 0, :, half(h)]
                )
                acc = plus_adjoint(acc, back)
            for c in range(18):
                w[c, s, :, half(h)] = acc[c]


def near_kernel(step, links, g, w, upz, upy, zh, yu, yd, th, *refs):
    refs = list(refs)
    before = [refs.pop(0), refs.pop(0)] if step.mode == TURN else [None, None]
    gn, wf = refs.pop(0), refs.pop(0)
    kept = [refs.pop(0), refs.pop(0)] if step.keeps else [None, None]
    tp = None if step.last else refs.pop(0)
    qn = refs.pop(0) if step.sends == TURN else None
    sums = refs.pop(0) if step.colour == 1 else None
    z_scr, y_scr = refs
    own = links.at[step.colour]
    if step.first:
        g = g.at[step.colour]
    core = lax.axis_index("tc")
    far, near = slices(core)
    row, lane = iotas()
    part = behind(
        step.mode, lambda c: zh[c], lambda c: pltpu.roll(upz[c], 4, 0), before[0]
    )
    for c in range(18):
        z_scr[c] = part[c]
        if kept[0] is not None:
            kept[0][c] = part[c]
    part = behind(
        step.mode,
        lambda c: received_rows(c, yu, yd),
        lambda c: pltpu.roll(upy[c], 64, 1),
        before[1],
    )
    for c in range(18):
        v = part[c]
        if kept[1] is not None:
            kept[1][c] = v
        for k in range(2):
            y_scr[c, k, :, half(0)] = jnp.where(lane < 32, pltpu.roll(v, 64 - 32 * k, 1), 0.0)
            y_scr[c, k, :, half(1)] = jnp.where(lane < 96, 0.0, pltpu.roll(v, 96 - 32 * k, 1))

    def with_sides(k, s, h):
        side = []
        for c in range(18):
            r = 2 * k + h
            up = jnp.broadcast_to(z_scr[c, r : r + 1, :], (8, 128))
            down = jnp.broadcast_to(z_scr[c, 4 + r : 5 + r, :], (8, 128))
            edge = jnp.where(row == 7, up, jnp.where(row == 0, down, 0.0))
            side.append(edge + y_scr[c, k, :, half(h)])
        return plus_adjoint([w[c, s, :, half(h)] for c in range(18)], side)

    total = None
    for h in range(2):
        acc = with_sides(0, far, h)
        for c in range(18):
            wf[c, :, half(h)] = acc[c]
        link = crossing(own, h, core == 1)
        acc = with_sides(1, near, h)
        acc = times_adjoint(acc, link, lambda c: th[c, :, half(h)])
        new, mat, turn = relax([g[c, near, :, half(h)] for c in range(18)], acc)
        for c in range(18):
            gn[c, :, half(h)] = new[c]
        if tp is not None:
            face = times(lambda c: new[c], link)
            for c in range(18):
                tp[c, :, half(h)] = face[c]
        if qn is not None:
            for k in range(12):
                qn[k, :, half(h)] = turn[k]
        if sums is not None:
            now = measures(mat)
            total = now if total is None else [a + b for a, b in zip(total, now)]
    if sums is not None:
        sums[0] = total[0]
        sums[1] = total[1]


def far_kernel(step, links, g, gn, wf, fh, *refs):
    refs = list(refs)
    before = refs.pop(0) if step.mode == TURN else None
    near_sums = refs.pop(0) if step.colour == 1 else None
    line = refs.pop(0) if step.colour == 1 and step.number > 1 else None
    g0 = refs.pop(0) if step.last else None
    upz = refs.pop(0) if step.sends == WHOLE else None
    upy = refs.pop(0) if step.sends == WHOLE else None
    qn = refs.pop(0) if step.sends == TURN else None
    out = refs.pop(0)
    kept = refs.pop(0) if step.keeps else None
    fp, zp, lowp, highp = [None] * 4 if step.last else [refs.pop(0) for _ in range(4)]
    sums = refs.pop(0) if step.colour == 1 else None
    own = links.at[step.colour]
    if step.first:
        g = g.at[step.colour]
    core = lax.axis_index("tc")
    far, near = slices(core)
    total = None if sums is None else [near_sums[0], near_sums[1]]
    to = out.at[1] if step.last else out
    for h in range(2):
        link = crossing(own, h, core == 0)
        part = behind(
            step.mode,
            lambda c: fh[c, :, half(h)],
            link,
            None if before is None else [before[c, :, half(h)] for c in range(18)],
        )
        if kept is not None:
            for c in range(18):
                kept[c, :, half(h)] = part[c]
        acc = plus_adjoint([wf[c, :, half(h)] for c in range(18)], part)
        new, mat, turn = relax([g[c, far, :, half(h)] for c in range(18)], acc)
        for c in range(18):
            to[c, far, :, half(h)] = new[c]
        if step.sends == WHOLE:
            face = times(lambda c: new[c], link)
            for c in range(18):
                fp[c, :, half(h)] = face[c]
        if step.sends == TURN:
            for k in range(12):
                fp[k, :, half(h)] = turn[k]
                pack_rows(k, 0, turn[k], h, zp)
                pack_rows(k, 1, qn[k, :, half(h)], h, zp)
        if sums is not None:
            total = [a + b for a, b in zip(total, measures(mat))]
    for c in range(18):
        to[c, near] = gn[c]
    if step.last:
        for c in range(18):
            for s in range(2):
                out[0, c, s] = g0[c, s]
    else:
        if step.sends == WHOLE:
            pack_z(core, out, upz, zp, refs.pop(0))
            pack_y(core, out, upy, lowp, highp)
        else:
            ends = [row_ends(lambda j, h: (fp, qn)[j][k, :, half(h)]) for k in range(12)]
            send_rows(ends, lowp, highp)
    if sums is not None:
        lane = lax.broadcasted_iota(jnp.int32, (1, 128), 1)
        line = jnp.zeros((1, 128), F32) if line is None else line[...]
        for k in range(2):
            rows = jnp.sum(total[k], axis=0, keepdims=True)
            value = jnp.sum(rows, axis=1, keepdims=True)
            line = jnp.where(lane == ITERS * k + step.number // 2, value, line)
        sums[...] = line


def final_kernel(volume, parts, monitor):
    total = jnp.sum(parts[...], axis=0)
    both = jnp.concatenate([total, pltpu.roll(total, 128 - ITERS, 1)], axis=0)
    row = lax.broadcasted_iota(jnp.int32, (2, 128), 0)
    both = jnp.where(row == 0, 1.0 - both / (12.0 * volume), both / (volume / 2.0))
    monitor[...] = both[:, :ITERS]


def call(body, outs, scratch, args, flops, space=pltpu.VMEM):
    return pl.pallas_call(
        body,
        out_shape=[jax.ShapeDtypeStruct(o, F32) for o in outs],
        in_specs=[pl.BlockSpec(memory_space=space)] * len(args),
        out_specs=[pl.BlockSpec(memory_space=pltpu.VMEM)] * len(outs),
        scratch_shapes=[s if not isinstance(s, tuple) else pltpu.VMEM(s, F32) for s in scratch],
        compiler_params=pltpu.CompilerParams(vmem_limit_bytes=24 * 2**20),
        cost_estimate=pl.CostEstimate(flops=flops, bytes_accessed=0, transcendentals=0),
    )(*args)


def swap(value, axis, partner):
    count = lax.axis_size(axis)
    return lax.ppermute(value, axis, [(i, partner(i) % count) for i in range(count)])


def even_odd(i):
    return i ^ 1


def odd_even(i):
    return i + 1 if i % 2 else i - 1


FACE = (18, 8, 256)
SIDE = (18, 8, 128)
FIELD = (18, 2, 8, 256)
FACE_12 = (12, 8, 256)
SIDE_12 = (12, 8, 128)
ROW = (9, 8, 128)
ROW_12 = (6, 8, 128)
SUMS = (2, 8, 128)
SENT = {WHOLE: [FACE, SIDE, ROW, ROW], TURN: [FACE_12, SIDE_12, ROW_12, ROW_12]}


class Step:
    def __init__(self, number):
        self.number = number
        self.colour = number % 2
        self.first = number < 2
        self.last = number == 2 * ITERS - 1
        self.mode = TWO_ROWS if number == 0 else WHOLE if number == 1 else TURN
        self.keeps = number < 2 * ITERS - 2
        self.sends = None if self.last else WHOLE if number == 0 else TURN


def shards(lattice_links, transform):
    volume = 2 * transform.shape[2] * transform.shape[3] * transform.shape[4]
    for axis in AXES:
        volume *= lax.axis_size(axis)
    links, start, tp, fp, zp, lowp, highp, *sides = call(
        first_kernel,
        [lattice_links.shape, transform.shape, FACE, FACE_12, SIDE_12, ROW_12, ROW_12]
        + [SIDE] * 4,
        [SIDE, pltpu.SemaphoreType.DMA((10,))],
        [pltpu.with_memory_space_constraint(v, pltpu.HBM) for v in (lattice_links, transform)],
        10**7,
        pltpu.HBM,
    )
    g = [start, start]
    packed = [sides[:2], sides[2:]]
    kept_far, kept_side = [None, None], [None, None]
    th = swap(tp, "tc", even_odd)
    line = None
    for step in map(Step, range(2 * ITERS)):
        colour = step.colour
        fh = swap(fp, TA, odd_even)
        yu = swap(lowp, "gy", lambda i: i - 1)
        yd = swap(highp, "gy", lambda i: i + 1)
        zh = swap(zp, "gz", even_odd)
        (w,) = call(
            functools.partial(local_kernel, colour, step.number == 0),
            [FIELD],
            [],
            [links, g[1 - colour]],
            3 * 10**7,
        )
        outs = [FACE, FACE]
        outs += [SIDE, SIDE] if step.keeps else []
        outs += [] if step.last else [FACE]
        outs += [FACE_12] if step.sends == TURN else []
        outs += [SUMS] if colour == 1 else []
        args = [links, g[colour], w, *packed[colour], zh, yu, yd, th]
        args += kept_side[colour] if step.mode == TURN else []
        gn, wf, *rest = call(functools.partial(near_kernel, step), outs, [SIDE, FIELD], args, 10**7)
        if step.keeps:
            kept_side[colour] = [rest.pop(0), rest.pop(0)]
        if not step.last:
            th = swap(rest.pop(0), "tc", even_odd)
        args = [links, g[colour], gn, wf, fh]
        args += [kept_far[colour]] if step.mode == TURN else []
        args += [rest.pop()] if colour == 1 else []
        args += [line] if line is not None and colour == 1 else []
        args += [g[0]] if step.last else []
        args += packed[colour] if step.sends == WHOLE else []
        args += [rest.pop()] if step.sends == TURN else []
        outs = [(2,) + FIELD] if step.last else [FIELD]
        outs += [FACE] if step.keeps else []
        if not step.last:
            outs += SENT[step.sends]
        outs += [(1, 128)] if colour == 1 else []
        out, *rest = call(
            functools.partial(far_kernel, step),
            outs,
            [SIDE] if step.sends == WHOLE else [],
            args,
            10**7,
        )
        g[colour] = out
        if step.keeps:
            kept_far[colour] = rest.pop(0)
        if not step.last:
            fp, zp, lowp, highp, *rest = rest
        if colour == 1:
            (line,) = rest
    count = 1
    for axis in AXES:
        count *= lax.axis_size(axis)
    parts = jnp.broadcast_to(line[None], (count, 1, 128))
    parts = lax.all_to_all(parts, AXES, 0, 0, tiled=True)
    (monitor,) = call(functools.partial(final_kernel, volume), [(2, ITERS)], [], [parts], 10**3)
    return (out, monitor)


def solution(mesh):
    finer = Mesh(
        mesh.devices.reshape(8, 2, 2, mesh.shape["gz"], mesh.shape["gy"]),
        AXES,
    )
    return jax.shard_map(
        shards,
        mesh=finer,
        in_specs=(P(None, None, None, TA, "gz", "gy"), P(None, None, TA, "gz", "gy")),
        out_specs=(P(None, None, TA, "gz", "gy"), P()),
        check_vma=False,
    )
```

```python
import functools

import jax
import jax.numpy as jnp
from jax import lax
from jax.experimental import pallas as pl
from jax.experimental.pallas import tpu as pltpu
from jax.sharding import Mesh
from jax.sharding import PartitionSpec as P


ITERS = 2
OMEGA = 1.7
GUARD = 1e-12
TA = ("tz", "tx", "tc")
AXES = TA + ("gz", "gy")
F32 = jnp.float32
R3 = range(3)
PAIRS = ((0, 1), (0, 2), (1, 2))
ROWS = (0, 1, 2, 3, 4, 5, 9, 10, 11, 12, 13, 14)
TWO_ROWS, WHOLE, TURN = range(3)


def re(i, j):
    return 3 * i + j


def im(i, j):
    return 9 + 3 * i + j


def half(h):
    return pl.ds(128 * h, 128)


def times_adjoint(acc, left, right):
    out = list(acc)
    for k in R3:
        lr = [left(re(i, k)) for i in R3]
        li = [left(im(i, k)) for i in R3]
        rr = [right(re(j, k)) for j in R3]
        ri = [right(im(j, k)) for j in R3]
        for i in R3:
            for j in R3:
                tr = lr[i] * rr[j] + li[i] * ri[j]
                ti = li[i] * rr[j] - lr[i] * ri[j]
                a, b = re(i, j), im(i, j)
                out[a] = tr if out[a] is None else out[a] + tr
                out[b] = ti if out[b] is None else out[b] + ti
    return out


def times(left, right):
    out = [None] * 18
    for k in R3:
        lr = [left(re(i, k)) for i in R3]
        li = [left(im(i, k)) for i in R3]
        rr = [right(re(k, j)) for j in R3]
        ri = [right(im(k, j)) for j in R3]
        for i in R3:
            for j in R3:
                tr = lr[i] * rr[j] - li[i] * ri[j]
                ti = lr[i] * ri[j] + li[i] * rr[j]
                a, b = re(i, j), im(i, j)
                out[a] = tr if out[a] is None else out[a] + tr
                out[b] = ti if out[b] is None else out[b] + ti
    return out


def plus_adjoint(acc, mat):
    out = list(acc)
    for i in R3:
        for j in R3:
            out[re(i, j)] = out[re(i, j)] + mat[re(j, i)]
            out[im(i, j)] = out[im(i, j)] - mat[im(j, i)]
    return out


def rotation(a, p, q):
    v0 = a[re(p, p)] + a[re(q, q)]
    v1 = -(a[im(p, q)] + a[im(q, p)])
    v2 = a[re(q, p)] - a[re(p, q)]
    v3 = -(a[im(p, p)] - a[im(q, q)])
    length = jnp.sqrt(v0 * v0 + v1 * v1 + v2 * v2 + v3 * v3)
    s0 = (1.0 - OMEGA) * length + OMEGA * v0
    s1, s2, s3 = OMEGA * v1, OMEGA * v2, OMEGA * v3
    inverse = lax.rsqrt(s0 * s0 + s1 * s1 + s2 * s2 + s3 * s3 + GUARD)
    return s0 * inverse, s1 * inverse, s2 * inverse, s3 * inverse


def rotate(m, quat, p, q):
    q0, q1, q2, q3 = quat
    out = list(m)
    for j in R3:
        ur, ui = m[re(p, j)], m[im(p, j)]
        lr, li = m[re(q, j)], m[im(q, j)]
        out[re(p, j)] = q0 * ur - q3 * ui + q2 * lr - q1 * li
        out[im(p, j)] = q0 * ui + q3 * ur + q2 * li + q1 * lr
        out[re(q, j)] = q0 * lr + q3 * li - q2 * ur - q1 * ui
        out[im(q, j)] = q0 * li - q3 * lr - q2 * ui + q1 * ur
    return out


def relax(g, w):
    a = times(lambda c: g[c], lambda c: w[c])
    turn = []
    for p, q in PAIRS:
        quat = rotation(a, p, q)
        a = rotate(a, quat, p, q)
        g = rotate(g, quat, p, q)
        turn += quat
    return g, a, turn


def turned(mat, turn):
    for k, (p, q) in enumerate(PAIRS):
        mat = rotate(mat, turn[4 * k : 4 * k + 4], p, q)
    return mat


def third_row(rows):
    a = [None] * 18
    for c, v in zip(ROWS, rows):
        a[c] = v
    for j in R3:
        k, m = (j + 1) % 3, (j + 2) % 3
        ur, ui, xr, xi = a[re(0, k)], a[im(0, k)], a[re(1, m)], a[im(1, m)]
        vr, vi, yr, yi = a[re(0, m)], a[im(0, m)], a[re(1, k)], a[im(1, k)]
        a[re(2, j)] = (ur * xr - ui * xi) - (vr * yr - vi * yi)
        a[im(2, j)] = (vr * yi + vi * yr) - (ur * xi + ui * xr)
    return a


def behind(mode, sent, link, before):
    if mode == TURN:
        return turned([before[c] for c in range(18)], [sent(c) for c in range(12)])
    if mode == TWO_ROWS:
        full = third_row([sent(k) for k in range(12)])
        return times_adjoint([None] * 18, lambda c: full[c], link)
    return times_adjoint([None] * 18, sent, link)


def measures(a):
    func = a[re(0, 0)] + a[re(1, 1)] + a[re(2, 2)]
    off = None
    for i, j in PAIRS:
        dr = a[re(i, j)] - a[re(j, i)]
        di = a[im(i, j)] + a[im(j, i)]
        term = dr * dr + di * di
        off = term if off is None else off + term
    mean = (a[im(0, 0)] + a[im(1, 1)] + a[im(2, 2)]) / 3.0
    div = 0.5 * off
    for i in R3:
        d = a[im(i, i)] - mean
        div = div + d * d
    return func, div


def unit(c):
    return 1.0 if c in (0, 4, 8) else 0.0


def crossing(links, h, is_unit):
    return lambda c: jnp.where(is_unit, F32(unit(c)), links[3, c, 1, :, half(h)])


def iotas():
    return (
        lax.broadcasted_iota(jnp.int32, (8, 128), 0),
        lax.broadcasted_iota(jnp.int32, (8, 128), 1),
    )


def slices(core):
    return core, 1 - core


def pack_links(core, links, upz, upy):
    _, lane = iotas()
    for c in range(18):
        upz[c] = jnp.full((8, 128), unit(c), F32)
        for k, s in enumerate(slices(core)):
            for h in range(2):
                r = 4 + 2 * k + h
                upz[c, r : r + 1, :] = links[2, c, s, 7:8, half(h)]
        high0 = pltpu.roll(links[1, c, core, :, half(1)], 96, 1)
        high1 = links[1, c, 1 - core, :, half(1)]
        upy[c] = jnp.where(lane < 64, F32(unit(c)), jnp.where(lane < 96, high0, high1))


def pack_rows(c, k, value, h, scr):
    scr[c, 2 * k + h : 2 * k + h + 1, :] = value[0:1, :]
    scr[c, 4 + 2 * k + h : 5 + 2 * k + h, :] = value[7:8, :]


def pack_z(core, g, upz, zp, scr):
    for c in range(18):
        for k, s in enumerate(slices(core)):
            for h in range(2):
                pack_rows(c, k, g[c, s, :, half(h)], h, scr)
    out = times(lambda c: scr[c], lambda c: upz[c])
    for k, c in enumerate(ROWS if zp.shape[0] == 12 else range(18)):
        zp[k] = out[c]


def row_ends(value):
    _, lane = iotas()
    low1 = pltpu.roll(value(1, 0), 32, 1)
    high0 = pltpu.roll(value(0, 1), 96, 1)
    return jnp.where(
        lane < 64,
        jnp.where(lane < 32, value(0, 0), low1),
        jnp.where(lane < 96, high0, value(1, 1)),
    )


def send_rows(ends, lowp, highp):
    _, lane = iotas()
    for k in range(lowp.shape[0]):
        a, b = ends[2 * k], ends[2 * k + 1]
        lowp[k] = jnp.where(lane < 64, a, pltpu.roll(b, 64, 1))
        highp[k] = jnp.where(lane < 64, pltpu.roll(a, 64, 1), b)


def received_rows(c, yu, yd):
    _, lane = iotas()
    u, d = yu[c // 2], yd[c // 2]
    if c % 2:
        return jnp.where(lane < 64, pltpu.roll(u, 64, 1), d)
    return jnp.where(lane < 64, u, pltpu.roll(d, 64, 1))


def pack_y(core, g, upy, lowp, highp):
    ends = [
        row_ends(lambda k, h: g[c, slices(core)[k], :, half(h)]) for c in range(18)
    ]
    out = times(lambda c: ends[c], lambda c: upy[c])
    if lowp.shape[0] == 6:
        out = [out[c] for c in ROWS]
    send_rows(out, lowp, highp)


def first_kernel(links_hbm, g_hbm, tp, fp, zp, lowp, highp, upz, upy, scr, links, g, sems):
    right = pl.ds(128, 128)
    copies = [
        (g_hbm.at[1], g),
        (links_hbm.at[1, 3, :, 1], links.at[3, :, 1]),
        (links_hbm.at[1, 2], links.at[2]),
        (links_hbm.at[1, 1, :, :, :, right], links.at[1, :, :, :, right]),
    ]
    copies = [pltpu.make_async_copy(a, b, sems.at[k]) for k, (a, b) in enumerate(copies)]
    for copy in copies:
        copy.start()
    core = lax.axis_index("tc")
    far, near = slices(core)
    for copy in copies[:2]:
        copy.wait()
    for h in range(2):
        face = times(lambda c: g[c, far, :, half(h)], crossing(links, h, core == 0))
        for k, c in enumerate(ROWS):
            fp[k, :, half(h)] = face[c]
        face = times(lambda c: g[c, near, :, half(h)], crossing(links, h, core == 1))
        for c in range(18):
            tp[c, :, half(h)] = face[c]
    for copy in copies[2:]:
        copy.wait()
    pack_links(core, links, upz, upy)
    pack_z(core, g, upz, zp, scr)
    pack_y(core, g, upy, lowp, highp)


def local_kernel(step, links, gp, *refs):
    refs = list(refs)
    w = refs.pop(0)
    colour = step.colour
    if step.number == 0:
        pack_links(lax.axis_index("tc"), links.at[0], *refs)
    if step.last:
        out, sem = refs
        copy = pltpu.make_async_copy(gp, out.at[1 - colour], sem)
        copy.start()
    first = step.number == 0
    own, other = links.at[colour], links.at[1 - colour]
    if first:
        gp = gp.at[1 - colour]
    row, lane = iotas()
    column = lane % 32
    parity = (row + lane // 32) % 2
    for s in range(2):
        stays = parity == (s + colour) % 2
        behind = []
        for h in range(2):
            behind.append(
                times(lambda c: gp[c, s, :, half(h)], lambda c: other[1, c, s, :, half(h)])
            )
        low, high = [], []
        for c in range(18):
            r0 = pltpu.roll(behind[0][c], 32, 1)
            r1 = pltpu.roll(behind[1][c], 32, 1)
            low.append(jnp.where(lane < 32, 0.0, r0))
            high.append(jnp.where(lane < 32, r0, r1))
        for h, mat in ((0, low), (1, high)):
            acc = plus_adjoint([jnp.zeros((8, 128), F32)] * 18, mat)
            for c in range(18):
                w[c, s, :, half(h)] = acc[c]
        for h in range(2):
            acc = [w[c, s, :, half(h)] for c in range(18)]

            def tile(c):
                return gp[c, s, :, half(h)]

            def ahead_x(c):
                v = tile(c)
                moved = jnp.where(column == 31, pltpu.roll(v, 31, 1), pltpu.roll(v, 127, 1))
                return jnp.where(stays, v, moved)

            acc = times_adjoint(acc, lambda c: own[0, c, s, :, half(h)], ahead_x)

            def ahead_y(c):
                a = pltpu.roll(gp[c, s, :, half(1)], 96, 1)
                if h == 0:
                    return jnp.where(lane >= 96, a, pltpu.roll(tile(c), 96, 1))
                return jnp.where(lane >= 96, 0.0, a)

            acc = times_adjoint(acc, lambda c: own[1, c, s, :, half(h)], ahead_y)

            def ahead_z(c):
                return jnp.where(row == 7, 0.0, pltpu.roll(tile(c), 7, 0))

            acc = times_adjoint(acc, lambda c: own[2, c, s, :, half(h)], ahead_z)
            back = times(tile, lambda c: other[0, c, s, :, half(h)])
            shifted = []
            for v in back:
                moved = jnp.where(column == 0, pltpu.roll(v, 97, 1), pltpu.roll(v, 1, 1))
                shifted.append(jnp.where(stays, moved, v))
            acc = plus_adjoint(acc, shifted)
            back = times(tile, lambda c: other[2, c, s, :, half(h)])
            acc = plus_adjoint(acc, [jnp.where(row == 0, 0.0, pltpu.roll(v, 1, 0)) for v in back])
            if s == 0:
                acc = times_adjoint(
                    acc,
                    lambda c: own[3, c, 0, :, half(h)],
                    lambda c: gp[c, 1, :, half(h)],
                )
            else:
                back = times(
                    lambda c: gp[c, 0, :, half(h)], lambda c: other[3, c, 0, :, half(h)]
                )
                acc = plus_adjoint(acc, back)
            for c in range(18):
                w[c, s, :, half(h)] = acc[c]
    if step.last:
        copy.wait()


def near_kernel(step, links, g, w, upz, upy, zh, yu, yd, th, *refs):
    refs = list(refs)
    before = [refs.pop(0), refs.pop(0)] if step.mode == TURN else [None, None]
    gn, wf = refs.pop(0), refs.pop(0)
    kept = [refs.pop(0), refs.pop(0)] if step.keeps else [None, None]
    tp = None if step.last else refs.pop(0)
    qn = refs.pop(0) if step.sends == TURN else None
    sums = refs.pop(0) if step.colour == 1 else None
    z_scr, y_scr = refs
    own = links.at[step.colour]
    if step.first:
        g = g.at[step.colour]
    core = lax.axis_index("tc")
    far, near = slices(core)
    row, lane = iotas()
    part = behind(
        step.mode, lambda c: zh[c], lambda c: pltpu.roll(upz[c], 4, 0), before[0]
    )
    for c in range(18):
        z_scr[c] = part[c]
        if kept[0] is not None:
            kept[0][c] = part[c]
    part = behind(
        step.mode,
        lambda c: received_rows(c, yu, yd),
        lambda c: pltpu.roll(upy[c], 64, 1),
        before[1],
    )
    for c in range(18):
        v = part[c]
        if kept[1] is not None:
            kept[1][c] = v
        for k in range(2):
            y_scr[c, k, :, half(0)] = jnp.where(lane < 32, pltpu.roll(v, 64 - 32 * k, 1), 0.0)
            y_scr[c, k, :, half(1)] = jnp.where(lane < 96, 0.0, pltpu.roll(v, 96 - 32 * k, 1))

    def with_sides(k, s, h):
        side = []
        for c in range(18):
            r = 2 * k + h
            up = jnp.broadcast_to(z_scr[c, r : r + 1, :], (8, 128))
            down = jnp.broadcast_to(z_scr[c, 4 + r : 5 + r, :], (8, 128))
            edge = jnp.where(row == 7, up, jnp.where(row == 0, down, 0.0))
            side.append(edge + y_scr[c, k, :, half(h)])
        return plus_adjoint([w[c, s, :, half(h)] for c in range(18)], side)

    total = None
    for h in range(2):
        acc = with_sides(0, far, h)
        for c in range(18):
            wf[c, :, half(h)] = acc[c]
        link = crossing(own, h, core == 1)
        acc = with_sides(1, near, h)
        acc = times_adjoint(acc, link, lambda c: th[c, :, half(h)])
        new, mat, turn = relax([g[c, near, :, half(h)] for c in range(18)], acc)
        for c in range(18):
            gn[c, :, half(h)] = new[c]
        if tp is not None:
            face = times(lambda c: new[c], link)
            for c in range(18):
                tp[c, :, half(h)] = face[c]
        if qn is not None:
            for k in range(12):
                qn[k, :, half(h)] = turn[k]
        if sums is not None:
            now = measures(mat)
            total = now if total is None else [a + b for a, b in zip(total, now)]
    if sums is not None:
        sums[0] = total[0]
        sums[1] = total[1]


def far_kernel(step, links, g, gn, wf, fh, *refs):
    refs = list(refs)
    before = refs.pop(0) if step.mode == TURN else None
    near_sums = refs.pop(0) if step.colour == 1 else None
    line = refs.pop(0) if step.colour == 1 and step.number > 1 else None
    upz = refs.pop(0) if step.sends == WHOLE else None
    upy = refs.pop(0) if step.sends == WHOLE else None
    qn = refs.pop(0) if step.sends == TURN else None
    out = refs.pop(0)
    kept = refs.pop(0) if step.keeps else None
    fp, zp, lowp, highp = [None] * 4 if step.last else [refs.pop(0) for _ in range(4)]
    sums = refs.pop(0) if step.colour == 1 else None
    own = links.at[step.colour]
    if step.first:
        g = g.at[step.colour]
    core = lax.axis_index("tc")
    far, near = slices(core)
    total = None if sums is None else [near_sums[0], near_sums[1]]
    for h in range(2):
        link = crossing(own, h, core == 0)
        part = behind(
            step.mode,
            lambda c: fh[c, :, half(h)],
            link,
            None if before is None else [before[c, :, half(h)] for c in range(18)],
        )
        if kept is not None:
            for c in range(18):
                kept[c, :, half(h)] = part[c]
        acc = plus_adjoint([wf[c, :, half(h)] for c in range(18)], part)
        new, mat, turn = relax([g[c, far, :, half(h)] for c in range(18)], acc)
        for c in range(18):
            if step.last:
                out[c, :, half(h)] = new[c]
            else:
                out[c, far, :, half(h)] = new[c]
        if step.sends == WHOLE:
            face = times(lambda c: new[c], link)
            for c in range(18):
                fp[c, :, half(h)] = face[c]
        if step.sends == TURN:
            for k in range(12):
                fp[k, :, half(h)] = turn[k]
                pack_rows(k, 0, turn[k], h, zp)
                pack_rows(k, 1, qn[k, :, half(h)], h, zp)
        if sums is not None:
            total = [a + b for a, b in zip(total, measures(mat))]
    if not step.last:
        for c in range(18):
            out[c, near] = gn[c]
        if step.sends == WHOLE:
            pack_z(core, out, upz, zp, refs.pop(0))
            pack_y(core, out, upy, lowp, highp)
        else:
            ends = [row_ends(lambda j, h: (fp, qn)[j][k, :, half(h)]) for k in range(12)]
            send_rows(ends, lowp, highp)
    if sums is not None:
        lane = lax.broadcasted_iota(jnp.int32, (1, 128), 1)
        line = jnp.zeros((1, 128), F32) if line is None else line[...]
        for k in range(2):
            rows = jnp.sum(total[k], axis=0, keepdims=True)
            value = jnp.sum(rows, axis=1, keepdims=True)
            line = jnp.where(lane == ITERS * k + step.number // 2, value, line)
        sums[...] = line


def final_kernel(volume, parts, gn, gf, begun, out, monitor, scr, sems):
    copies = [
        pltpu.make_async_copy(part, out.at[1, :, s], sems.at[k])
        for k, (part, s) in enumerate(zip((gf, gn), slices(lax.axis_index("tc"))))
    ]
    for copy in copies:
        copy.start()
    total = parts[0]
    for k in range(1, parts.shape[0]):
        total = total + parts[k]
    total = jnp.sum(total, axis=0, keepdims=True)
    both = jnp.concatenate([total, pltpu.roll(total, 128 - ITERS, 1)], axis=0)
    row = lax.broadcasted_iota(jnp.int32, (2, 128), 0)
    both = jnp.where(row == 0, 1.0 - both / (12.0 * volume), both / (volume / 2.0))
    scr[...] = both[:, :ITERS]
    copies.append(pltpu.make_async_copy(scr, monitor, sems.at[2]))
    copies[2].start()
    for copy in copies:
        copy.wait()


def call(body, outs, scratch, args, flops, hbm=False, hbm_outs=(), aliases={}):
    return pl.pallas_call(
        body,
        out_shape=[jax.ShapeDtypeStruct(o, F32) for o in outs],
        in_specs=[
            pl.BlockSpec(memory_space=pltpu.HBM if hbm or k in aliases else pltpu.VMEM)
            for k in range(len(args))
        ],
        out_specs=[
            pl.BlockSpec(memory_space=pltpu.HBM if k in hbm_outs else pltpu.VMEM)
            for k in range(len(outs))
        ],
        scratch_shapes=[s if not isinstance(s, tuple) else pltpu.VMEM(s, F32) for s in scratch],
        compiler_params=pltpu.CompilerParams(vmem_limit_bytes=24 * 2**20),
        cost_estimate=pl.CostEstimate(flops=flops, bytes_accessed=0, transcendentals=0),
        input_output_aliases=aliases,
    )(*args)


def swap(value, axis, partner):
    count = lax.axis_size(axis)
    return lax.ppermute(value, axis, [(i, partner(i) % count) for i in range(count)])


def even_odd(i):
    return i ^ 1


def odd_even(i):
    return i + 1 if i % 2 else i - 1


FACE = (18, 8, 256)
SIDE = (18, 8, 128)
FIELD = (18, 2, 8, 256)
FACE_12 = (12, 8, 256)
SIDE_12 = (12, 8, 128)
ROW = (9, 8, 128)
ROW_12 = (6, 8, 128)
SUMS = (2, 8, 128)
SENT = {WHOLE: [FACE, SIDE, ROW, ROW], TURN: [FACE_12, SIDE_12, ROW_12, ROW_12]}


class Step:
    def __init__(self, number):
        self.number = number
        self.colour = number % 2
        self.first = number < 2
        self.last = number == 2 * ITERS - 1
        self.mode = TWO_ROWS if number == 0 else WHOLE if number == 1 else TURN
        self.keeps = number < 2 * ITERS - 2
        self.sends = None if self.last else WHOLE if number == 0 else TURN


def shards(lattice_links, transform):
    volume = 2 * transform.shape[2] * transform.shape[3] * transform.shape[4]
    for axis in AXES:
        volume *= lax.axis_size(axis)
    tp, fp, zp, lowp, highp, *side = call(
        first_kernel,
        [FACE, FACE_12, SIDE_12, ROW_12, ROW_12, SIDE, SIDE],
        [SIDE, (4,) + FIELD, FIELD, pltpu.SemaphoreType.DMA((4,))],
        [pltpu.with_memory_space_constraint(v, pltpu.HBM) for v in (lattice_links, transform)],
        10**7,
        hbm=True,
    )
    links = lattice_links
    g = [transform, transform]
    packed = [None, side]
    kept_far, kept_side = [None, None], [None, None]
    line = None
    for step in map(Step, range(2 * ITERS)):
        colour = step.colour
        fh = swap(fp, TA, odd_even)
        yu = swap(lowp, "gy", lambda i: i - 1)
        yd = swap(highp, "gy", lambda i: i + 1)
        zh = swap(zp, "gz", even_odd)
        th = swap(tp, "tc", even_odd)
        outs, scratch = [FIELD], []
        if step.number == 0:
            outs += [SIDE, SIDE]
        if step.last:
            outs += [(2,) + FIELD]
            scratch = [pltpu.SemaphoreType.DMA(())]
        w, *rest = call(
            functools.partial(local_kernel, step),
            outs,
            scratch,
            [links, g[1 - colour]],
            3 * 10**7,
            hbm_outs=(1,) if step.last else (),
        )
        if step.number == 0:
            packed[0] = rest
        if step.last:
            (begun,) = rest
        outs = [FACE, FACE]
        outs += [SIDE, SIDE] if step.keeps else []
        outs += [] if step.last else [FACE]
        outs += [FACE_12] if step.sends == TURN else []
        outs += [SUMS] if colour == 1 else []
        args = [links, g[colour], w, *packed[colour], zh, yu, yd, th]
        args += kept_side[colour] if step.mode == TURN else []
        gn, wf, *rest = call(functools.partial(near_kernel, step), outs, [SIDE, FIELD], args, 10**7)
        if step.keeps:
            kept_side[colour] = [rest.pop(0), rest.pop(0)]
        if not step.last:
            tp = rest.pop(0)
        args = [links, g[colour], gn, wf, fh]
        args += [kept_far[colour]] if step.mode == TURN else []
        args += [rest.pop()] if colour == 1 else []
        args += [line] if line is not None and colour == 1 else []
        args += packed[colour] if step.sends == WHOLE else []
        args += [rest.pop()] if step.sends == TURN else []
        outs = [FACE] if step.last else [FIELD]
        outs += [FACE] if step.keeps else []
        if not step.last:
            outs += SENT[step.sends]
        outs += [(1, 128)] if colour == 1 else []
        out, *rest = call(
            functools.partial(far_kernel, step),
            outs,
            [SIDE] if step.sends == WHOLE else [],
            args,
            10**7,
        )
        g[colour] = out
        if step.keeps:
            kept_far[colour] = rest.pop(0)
        if not step.last:
            fp, zp, lowp, highp, *rest = rest
        if colour == 1:
            (line,) = rest
    count = 1
    for axis in AXES:
        count *= lax.axis_size(axis)
    parts = jnp.broadcast_to(line[None], (count, 1, 128))
    parts = lax.all_to_all(parts, AXES, 0, 0, tiled=True).reshape(count // 8, 8, 128)
    out, monitor = call(
        functools.partial(final_kernel, volume),
        [(2,) + FIELD, (2, ITERS)],
        [(2, ITERS), pltpu.SemaphoreType.DMA((3,))],
        [parts, gn, out, begun],
        10**3,
        hbm_outs=(0, 1),
        aliases={3: 0},
    )
    return (out, monitor)


def solution(mesh):
    finer = Mesh(
        mesh.devices.reshape(8, 2, 2, mesh.shape["gz"], mesh.shape["gy"]),
        AXES,
    )
    return jax.shard_map(
        shards,
        mesh=finer,
        in_specs=(P(None, None, None, TA, "gz", "gy"), P(None, None, TA, "gz", "gy")),
        out_specs=(P(None, None, TA, "gz", "gy"), P()),
        check_vma=False,
    )
```

```python
import functools
import types

import jax
import jax.numpy as jnp
from jax import lax
from jax.experimental import pallas as pl
from jax.experimental.pallas import tpu as pltpu
from jax.sharding import Mesh
from jax.sharding import PartitionSpec as P


ITERS = 2
OMEGA = 1.7
GUARD = 1e-12
TA = ("tz", "tx", "tc")
AXES = TA + ("gz", "gy")
F32 = jnp.float32
R3 = range(3)
PAIRS = ((0, 1), (0, 2), (1, 2))
ROWS = (0, 1, 2, 3, 4, 5, 9, 10, 11, 12, 13, 14)
TWO_ROWS, WHOLE, TURN = range(3)


def re(i, j):
    return 3 * i + j


def im(i, j):
    return 9 + 3 * i + j


def half(h):
    return pl.ds(128 * h, 128)


def times_adjoint(acc, left, right):
    out = list(acc)
    for k in R3:
        lr = [left(re(i, k)) for i in R3]
        li = [left(im(i, k)) for i in R3]
        rr = [right(re(j, k)) for j in R3]
        ri = [right(im(j, k)) for j in R3]
        for i in R3:
            for j in R3:
                tr = lr[i] * rr[j] + li[i] * ri[j]
                ti = li[i] * rr[j] - lr[i] * ri[j]
                a, b = re(i, j), im(i, j)
                out[a] = tr if out[a] is None else out[a] + tr
                out[b] = ti if out[b] is None else out[b] + ti
    return out


def times(left, right):
    out = [None] * 18
    for k in R3:
        lr = [left(re(i, k)) for i in R3]
        li = [left(im(i, k)) for i in R3]
        rr = [right(re(k, j)) for j in R3]
        ri = [right(im(k, j)) for j in R3]
        for i in R3:
            for j in R3:
                tr = lr[i] * rr[j] - li[i] * ri[j]
                ti = lr[i] * ri[j] + li[i] * rr[j]
                a, b = re(i, j), im(i, j)
                out[a] = tr if out[a] is None else out[a] + tr
                out[b] = ti if out[b] is None else out[b] + ti
    return out


def plus_adjoint(acc, mat):
    out = list(acc)
    for i in R3:
        for j in R3:
            out[re(i, j)] = out[re(i, j)] + mat[re(j, i)]
            out[im(i, j)] = out[im(i, j)] - mat[im(j, i)]
    return out


def rotation(a, p, q):
    v0 = a[re(p, p)] + a[re(q, q)]
    v1 = -(a[im(p, q)] + a[im(q, p)])
    v2 = a[re(q, p)] - a[re(p, q)]
    v3 = -(a[im(p, p)] - a[im(q, q)])
    length = jnp.sqrt(v0 * v0 + v1 * v1 + v2 * v2 + v3 * v3)
    s0 = (1.0 - OMEGA) * length + OMEGA * v0
    s1, s2, s3 = OMEGA * v1, OMEGA * v2, OMEGA * v3
    inverse = lax.rsqrt(s0 * s0 + s1 * s1 + s2 * s2 + s3 * s3 + GUARD)
    return s0 * inverse, s1 * inverse, s2 * inverse, s3 * inverse


def rotate(m, quat, p, q):
    q0, q1, q2, q3 = quat
    out = list(m)
    for j in R3:
        ur, ui = m[re(p, j)], m[im(p, j)]
        lr, li = m[re(q, j)], m[im(q, j)]
        out[re(p, j)] = q0 * ur - q3 * ui + q2 * lr - q1 * li
        out[im(p, j)] = q0 * ui + q3 * ur + q2 * li + q1 * lr
        out[re(q, j)] = q0 * lr + q3 * li - q2 * ur - q1 * ui
        out[im(q, j)] = q0 * li - q3 * lr - q2 * ui + q1 * ur
    return out


def relax(g, w):
    a = times(lambda c: g[c], lambda c: w[c])
    turn = []
    for p, q in PAIRS:
        quat = rotation(a, p, q)
        a = rotate(a, quat, p, q)
        g = rotate(g, quat, p, q)
        turn += quat
    return g, a, turn


def turned(mat, turn):
    for k, (p, q) in enumerate(PAIRS):
        mat = rotate(mat, turn[4 * k : 4 * k + 4], p, q)
    return mat


def third_row(rows):
    a = [None] * 18
    for c, v in zip(ROWS, rows):
        a[c] = v
    for j in R3:
        k, m = (j + 1) % 3, (j + 2) % 3
        ur, ui, xr, xi = a[re(0, k)], a[im(0, k)], a[re(1, m)], a[im(1, m)]
        vr, vi, yr, yi = a[re(0, m)], a[im(0, m)], a[re(1, k)], a[im(1, k)]
        a[re(2, j)] = (ur * xr - ui * xi) - (vr * yr - vi * yi)
        a[im(2, j)] = (vr * yi + vi * yr) - (ur * xi + ui * xr)
    return a


def behind(mode, sent, link, before):
    if mode == TURN:
        return turned([before[c] for c in range(18)], [sent(c) for c in range(12)])
    if mode == TWO_ROWS:
        full = third_row([sent(k) for k in range(12)])
        if link is None:
            return full
        return times_adjoint([None] * 18, lambda c: full[c], link)
    if link is None:
        return [sent(c) for c in range(18)]
    return times_adjoint([None] * 18, sent, link)


def measures(a):
    func = a[re(0, 0)] + a[re(1, 1)] + a[re(2, 2)]
    off = None
    for i, j in PAIRS:
        dr = a[re(i, j)] - a[re(j, i)]
        di = a[im(i, j)] + a[im(j, i)]
        term = dr * dr + di * di
        off = term if off is None else off + term
    mean = (a[im(0, 0)] + a[im(1, 1)] + a[im(2, 2)]) / 3.0
    div = 0.5 * off
    for i in R3:
        d = a[im(i, i)] - mean
        div = div + d * d
    return func, div


def unit(c):
    return 1.0 if c in (0, 4, 8) else 0.0


def crossing(links, h, is_unit):
    return lambda c: jnp.where(is_unit, F32(unit(c)), links[3, c, 1, :, half(h)])


def iotas():
    return (
        lax.broadcasted_iota(jnp.int32, (8, 128), 0),
        lax.broadcasted_iota(jnp.int32, (8, 128), 1),
    )


def slices(core):
    return core, 1 - core


def pack_links(core, links, upz, upy):
    _, lane = iotas()
    for c in range(18):
        upz[c] = jnp.full((8, 128), unit(c), F32)
        for k, s in enumerate(slices(core)):
            for h in range(2):
                r = 4 + 2 * k + h
                upz[c, r : r + 1, :] = links[2, c, s, 7:8, half(h)]
        high0 = pltpu.roll(links[1, c, core, :, half(1)], 96, 1)
        high1 = links[1, c, 1 - core, :, half(1)]
        upy[c] = jnp.where(lane < 64, F32(unit(c)), jnp.where(lane < 96, high0, high1))


def pack_rows(c, k, value, h, scr):
    scr[c, 2 * k + h : 2 * k + h + 1, :] = value[0:1, :]
    scr[c, 4 + 2 * k + h : 5 + 2 * k + h, :] = value[7:8, :]


def pack_z(core, g, upz, zp, scr):
    for c in range(18):
        for k, s in enumerate(slices(core)):
            for h in range(2):
                pack_rows(c, k, g[c, s, :, half(h)], h, scr)
    out = times(lambda c: scr[c], lambda c: upz[c])
    for k, c in enumerate(ROWS if zp.shape[0] == 12 else range(18)):
        zp[k] = out[c]


def row_ends(value):
    _, lane = iotas()
    low1 = pltpu.roll(value(1, 0), 32, 1)
    high0 = pltpu.roll(value(0, 1), 96, 1)
    return jnp.where(
        lane < 64,
        jnp.where(lane < 32, value(0, 0), low1),
        jnp.where(lane < 96, high0, value(1, 1)),
    )


def send_rows(ends, lowp, highp):
    _, lane = iotas()
    for k in range(lowp.shape[0]):
        a, b = ends[2 * k], ends[2 * k + 1]
        lowp[k] = jnp.where(lane < 64, a, pltpu.roll(b, 64, 1))
        highp[k] = jnp.where(lane < 64, pltpu.roll(a, 64, 1), b)


def received(message, c):
    tile = message[c // 2]
    return pltpu.roll(tile, 64, 1) if c % 2 else tile


def pack_y(core, g, upy, lowp, highp):
    ends = [
        row_ends(lambda k, h: g[c, slices(core)[k], :, half(h)]) for c in range(18)
    ]
    out = times(lambda c: ends[c], lambda c: upy[c])
    if lowp.shape[0] == 6:
        out = [out[c] for c in ROWS]
    send_rows(out, lowp, highp)


def first_kernel(links_hbm, g_hbm, tp, fp, zp, lowp, highp, upz, upy, scr, links, g, sems):
    right = pl.ds(128, 128)
    copies = [
        (g_hbm.at[1], g),
        (links_hbm.at[1, 3, :, 1], links.at[3, :, 1]),
        (links_hbm.at[1, 2], links.at[2]),
        (links_hbm.at[1, 1, :, :, :, right], links.at[1, :, :, :, right]),
    ]
    copies = [pltpu.make_async_copy(a, b, sems.at[k]) for k, (a, b) in enumerate(copies)]
    for copy in copies:
        copy.start()
    core = lax.axis_index("tc")
    far, near = slices(core)
    for copy in copies[:2]:
        copy.wait()
    for h in range(2):
        face = times(lambda c: g[c, far, :, half(h)], crossing(links, h, core == 0))
        for k, c in enumerate(ROWS):
            fp[k, :, half(h)] = face[c]
        face = times(lambda c: g[c, near, :, half(h)], crossing(links, h, core == 1))
        for c in range(18):
            tp[c, :, half(h)] = face[c]
    for copy in copies[2:]:
        copy.wait()
    pack_links(core, links, upz, upy)
    pack_z(core, g, upz, zp, scr)
    pack_y(core, g, upy, lowp, highp)


def local_kernel(step, links, gp, *refs):
    refs = list(refs)
    w = refs.pop(0)
    colour = step.colour
    if step.number == 0:
        pack_links(lax.axis_index("tc"), links.at[0], *refs)
    if step.last:
        out, sem = refs
        copy = pltpu.make_async_copy(gp, out.at[1 - colour], sem)
        copy.start()
    first = step.number == 0
    own, other = links.at[colour], links.at[1 - colour]
    if first:
        gp = gp.at[1 - colour]
    row, lane = iotas()
    column = lane % 32
    parity = (row + lane // 32) % 2
    for s in range(2):
        stays = parity == (s + colour) % 2
        behind = []
        for h in range(2):
            behind.append(
                times(lambda c: gp[c, s, :, half(h)], lambda c: other[1, c, s, :, half(h)])
            )
        low, high = [], []
        for c in range(18):
            r0 = pltpu.roll(behind[0][c], 32, 1)
            r1 = pltpu.roll(behind[1][c], 32, 1)
            low.append(jnp.where(lane < 32, 0.0, r0))
            high.append(jnp.where(lane < 32, r0, r1))
        for h, mat in ((0, low), (1, high)):
            acc = plus_adjoint([jnp.zeros((8, 128), F32)] * 18, mat)
            for c in range(18):
                w[c, s, :, half(h)] = acc[c]
        for h in range(2):
            acc = [w[c, s, :, half(h)] for c in range(18)]

            def tile(c):
                return gp[c, s, :, half(h)]

            def ahead_x(c):
                v = tile(c)
                moved = jnp.where(column == 31, pltpu.roll(v, 31, 1), pltpu.roll(v, 127, 1))
                return jnp.where(stays, v, moved)

            acc = times_adjoint(acc, lambda c: own[0, c, s, :, half(h)], ahead_x)

            def ahead_y(c):
                a = pltpu.roll(gp[c, s, :, half(1)], 96, 1)
                if h == 0:
                    return jnp.where(lane >= 96, a, pltpu.roll(tile(c), 96, 1))
                return jnp.where(lane >= 96, 0.0, a)

            acc = times_adjoint(acc, lambda c: own[1, c, s, :, half(h)], ahead_y)

            def ahead_z(c):
                return jnp.where(row == 7, 0.0, pltpu.roll(tile(c), 7, 0))

            acc = times_adjoint(acc, lambda c: own[2, c, s, :, half(h)], ahead_z)
            back = times(tile, lambda c: other[0, c, s, :, half(h)])
            shifted = []
            for v in back:
                moved = jnp.where(column == 0, pltpu.roll(v, 97, 1), pltpu.roll(v, 1, 1))
                shifted.append(jnp.where(stays, moved, v))
            acc = plus_adjoint(acc, shifted)
            back = times(tile, lambda c: other[2, c, s, :, half(h)])
            acc = plus_adjoint(acc, [jnp.where(row == 0, 0.0, pltpu.roll(v, 1, 0)) for v in back])
            if s == 0:
                acc = times_adjoint(
                    acc,
                    lambda c: own[3, c, 0, :, half(h)],
                    lambda c: gp[c, 1, :, half(h)],
                )
            else:
                back = times(
                    lambda c: gp[c, 0, :, half(h)], lambda c: other[3, c, 0, :, half(h)]
                )
                acc = plus_adjoint(acc, back)
            for c in range(18):
                w[c, s, :, half(h)] = acc[c]
    if step.last:
        copy.wait()


def half_kernel(step, h, r):
    own = r.links.at[step.colour]
    g = r.g.at[step.colour] if step.first else r.g
    core = lax.axis_index("tc")
    far, near = slices(core)
    row, lane = iotas()
    if h == 0:
        part = behind(
            step.mode,
            lambda c: r.zh[c],
            lambda c: pltpu.roll(r.upz[c], 4, 0),
            r.z_before if step.mode == TURN else None,
        )
        for c in range(18):
            r.z_side[c] = part[c]
        link = None
        edge, shift = lane < 32, 0
    else:
        link = None if step.mode == TURN else (lambda c: pltpu.roll(r.upy[c], 64, 1))
        edge, shift = lane >= 96, 96
    y_side = behind(
        step.mode,
        lambda c: received(r.y, c),
        link,
        r.y_before if step.mode == TURN else None,
    )
    if step.keeps:
        for c in range(18):
            r.y_kept[c] = y_side[c]

    def with_sides(k, s):
        side = []
        for c in range(18):
            n = 2 * k + h
            up = jnp.broadcast_to(r.z_side[c, n : n + 1, :], (8, 128))
            down = jnp.broadcast_to(r.z_side[c, 4 + n : 5 + n, :], (8, 128))
            across = y_side[c]
            if (shift - 32 * k) % 128:
                across = pltpu.roll(across, (shift - 32 * k) % 128, 1)
            across = jnp.where(edge, across, 0.0)
            side.append(jnp.where(row == 7, up, jnp.where(row == 0, down, 0.0)) + across)
        return plus_adjoint([r.w[c, s, :, half(h)] for c in range(18)], side)

    total = None
    for k, s in ((1, near), (0, far)):
        acc = with_sides(k, s)
        if k == 1:
            link = crossing(own, h, core == 1)
            acc = times_adjoint(acc, link, lambda c: r.th[c, :, half(h)])
        else:
            link = crossing(own, h, core == 0)
            part = behind(
                step.mode,
                lambda c: r.fh[c, :, half(h)],
                link,
                r.f_before if step.mode == TURN else None,
            )
            if step.keeps:
                for c in range(18):
                    r.f_kept[c] = part[c]
            acc = plus_adjoint(acc, part)
        new, mat, turn = relax([g[c, s, :, half(h)] for c in range(18)], acc)
        to = (r.new_f, r.new_n)[k]
        for c in range(18):
            to[c] = new[c]
        if not step.last and (k == 1 or step.sends == WHOLE):
            face = times(lambda c: new[c], link)
            to = r.face_n if k == 1 else r.face_f
            for c in range(18):
                to[c] = face[c]
        if step.sends == TURN:
            to = (r.turn_f, r.turn_n)[k]
            for c in range(12):
                to[c] = turn[c]
        if step.colour == 1:
            now = measures(mat)
            total = now if total is None else [a + b for a, b in zip(total, now)]
    if h == 0:
        if step.colour == 1:
            r.sums[0] = total[0]
            r.sums[1] = total[1]
        return
    if step.colour == 1:
        total = [total[0] + r.sums0[0], total[1] + r.sums0[1]]
        place = lax.broadcasted_iota(jnp.int32, (1, 128), 1)
        line = r.line_before[...] if step.number > 1 else jnp.zeros((1, 128), F32)
        for k in range(2):
            rows = jnp.sum(total[k], axis=0, keepdims=True)
            value = jnp.sum(rows, axis=1, keepdims=True)
            line = jnp.where(place == ITERS * k + step.number // 2, value, line)
        r.line[...] = line
    for k, s in ((0, far), (1, near)):
        for c in range(18):
            for j, part in ((0, (r.new_f0, r.new_n0)[k]), (1, (r.new_f, r.new_n)[k])):
                if step.last:
                    (r.out_f, r.out_n)[k][c, :, half(j)] = part[c]
                else:
                    r.out[c, s, :, half(j)] = part[c]
    if step.last:
        return
    for c in range(18):
        r.tp[c, :, half(0)] = r.face_n0[c]
        r.tp[c, :, half(1)] = r.face_n[c]
        if step.sends == WHOLE:
            r.fp[c, :, half(0)] = r.face_f0[c]
            r.fp[c, :, half(1)] = r.face_f[c]
    if step.sends == WHOLE:
        pack_z(core, r.out, r.upz, r.zp, r.pack_scr)
        pack_y(core, r.out, r.upy, r.lowp, r.highp)
        return
    turns = ((r.turn_f0, r.turn_f), (r.turn_n0, r.turn_n))
    for c in range(12):
        for k in range(2):
            for j in range(2):
                pack_rows(c, k, turns[k][j][c], j, r.zp)
                if k == 0:
                    r.fp[c, :, half(j)] = turns[k][j][c]
    ends = [row_ends(lambda k, j: turns[k][j][c]) for c in range(12)]
    send_rows(ends, r.lowp, r.highp)


def final_kernel(volume, parts, gn, gf, begun, out, monitor, scr, sems):
    copies = [
        pltpu.make_async_copy(part, out.at[1, :, s], sems.at[k])
        for k, (part, s) in enumerate(zip((gf, gn), slices(lax.axis_index("tc"))))
    ]
    for copy in copies:
        copy.start()
    total = parts[0]
    for k in range(1, parts.shape[0]):
        total = total + parts[k]
    total = jnp.sum(total, axis=0, keepdims=True)
    both = jnp.concatenate([total, pltpu.roll(total, 128 - ITERS, 1)], axis=0)
    row = lax.broadcasted_iota(jnp.int32, (2, 128), 0)
    both = jnp.where(row == 0, 1.0 - both / (12.0 * volume), both / (volume / 2.0))
    scr[...] = both[:, :ITERS]
    copies.append(pltpu.make_async_copy(scr, monitor, sems.at[2]))
    copies[2].start()
    for copy in copies:
        copy.wait()


def call(body, outs, scratch, args, flops, hbm=False, hbm_outs=(), aliases={}):
    return pl.pallas_call(
        body,
        out_shape=[jax.ShapeDtypeStruct(o, F32) for o in outs],
        in_specs=[
            pl.BlockSpec(memory_space=pltpu.HBM if hbm or k in aliases else pltpu.VMEM)
            for k in range(len(args))
        ],
        out_specs=[
            pl.BlockSpec(memory_space=pltpu.HBM if k in hbm_outs else pltpu.VMEM)
            for k in range(len(outs))
        ],
        scratch_shapes=[s if not isinstance(s, tuple) else pltpu.VMEM(s, F32) for s in scratch],
        compiler_params=pltpu.CompilerParams(vmem_limit_bytes=24 * 2**20),
        cost_estimate=pl.CostEstimate(flops=flops, bytes_accessed=0, transcendentals=0),
        input_output_aliases=aliases,
    )(*args)


def named(body, ins, outs, scratch):
    names = list(ins) + list(outs) + list(scratch)

    def kernel(*refs):
        body(types.SimpleNamespace(**dict(zip(names, refs))))

    results = call(kernel, list(outs.values()), list(scratch.values()), list(ins.values()), 10**7)
    return dict(zip(outs, results))


def swap(value, axis, partner):
    count = lax.axis_size(axis)
    return lax.ppermute(value, axis, [(i, partner(i) % count) for i in range(count)])


def even_odd(i):
    return i ^ 1


def odd_even(i):
    return i + 1 if i % 2 else i - 1


FACE = (18, 8, 256)
SIDE = (18, 8, 128)
FIELD = (18, 2, 8, 256)
FACE_12 = (12, 8, 256)
SIDE_12 = (12, 8, 128)
ROW = (9, 8, 128)
ROW_12 = (6, 8, 128)
SUMS = (2, 8, 128)
SENT = {WHOLE: [FACE, SIDE, ROW, ROW], TURN: [FACE_12, SIDE_12, ROW_12, ROW_12]}


class Step:
    def __init__(self, number):
        self.number = number
        self.colour = number % 2
        self.first = number < 2
        self.last = number == 2 * ITERS - 1
        self.mode = TWO_ROWS if number == 0 else WHOLE if number == 1 else TURN
        self.keeps = number < 2 * ITERS - 2
        self.sends = None if self.last else WHOLE if number == 0 else TURN


def shards(lattice_links, transform):
    volume = 2 * transform.shape[2] * transform.shape[3] * transform.shape[4]
    for axis in AXES:
        volume *= lax.axis_size(axis)
    tp, fp, zp, lowp, highp, *side = call(
        first_kernel,
        [FACE, FACE_12, SIDE_12, ROW_12, ROW_12, SIDE, SIDE],
        [SIDE, (4,) + FIELD, FIELD, pltpu.SemaphoreType.DMA((4,))],
        [pltpu.with_memory_space_constraint(v, pltpu.HBM) for v in (lattice_links, transform)],
        10**7,
        hbm=True,
    )
    links = lattice_links
    g = [transform, transform]
    packed = [None, side]
    kept = [None, None]
    line = None
    for step in map(Step, range(2 * ITERS)):
        colour = step.colour
        fh = swap(fp, TA, odd_even)
        yu = swap(lowp, "gy", lambda i: i - 1)
        yd = swap(highp, "gy", lambda i: i + 1)
        zh = swap(zp, "gz", even_odd)
        th = swap(tp, "tc", even_odd)
        outs, scratch = [FIELD], []
        if step.number == 0:
            outs += [SIDE, SIDE]
        if step.last:
            outs += [(2,) + FIELD]
            scratch = [pltpu.SemaphoreType.DMA(())]
        w, *rest = call(
            functools.partial(local_kernel, step),
            outs,
            scratch,
            [links, g[1 - colour]],
            3 * 10**7,
            hbm_outs=(1,) if step.last else (),
        )
        if step.number == 0:
            packed[0] = rest
        if step.last:
            (begun,) = rest
        base = {"links": links, "g": g[colour], "w": w, "th": th, "fh": fh}
        outs = {"new_f": SIDE, "new_n": SIDE}
        if step.keeps:
            outs |= {"y_kept": SIDE, "f_kept": SIDE}
        scratch = {}
        if not step.last:
            outs |= {"face_n": SIDE}
        if step.sends == WHOLE:
            outs |= {"face_f": SIDE}
        if step.sends == TURN:
            outs |= {"turn_f": SIDE_12, "turn_n": SIDE_12}
        ins = base | {"zh": zh, "y": yd, "upz": packed[colour][0]}
        if step.mode == TURN:
            ins |= kept[colour][0]
        left = named(
            functools.partial(half_kernel, step, 0),
            ins,
            outs | {"z_side": SIDE} | ({"sums": SUMS} if colour == 1 else {}),
            {},
        )
        ins = base | {"z_side": left["z_side"], "y": yu}
        if step.mode == TURN:
            ins |= kept[colour][1]
        if step.mode != TURN or step.sends == WHOLE:
            ins |= {"upy": packed[colour][1]}
        if step.sends == WHOLE:
            ins |= {"upz": packed[colour][0]}
        ins |= {
            name + "0": left[name]
            for name in ("new_f", "new_n", "face_n", "face_f", "turn_f", "turn_n", "sums")
            if name in left
        }
        if colour == 1 and line is not None:
            ins |= {"line_before": line}
        scratch = {k: v for k, v in outs.items() if not k.endswith("_kept")}
        outs = {k: v for k, v in outs.items() if k.endswith("_kept")}
        if step.last:
            outs |= {"out_f": FACE, "out_n": FACE}
        else:
            outs |= {"out": FIELD, "tp": FACE}
            outs |= dict(zip(("fp", "zp", "lowp", "highp"), SENT[step.sends]))
        if colour == 1:
            outs |= {"line": (1, 128)}
        if step.sends == WHOLE:
            scratch |= {"pack_scr": SIDE}
        right = named(functools.partial(half_kernel, step, 1), ins, outs, scratch)
        if step.keeps:
            kept[colour] = [
                {"y_before": left["y_kept"], "f_before": left["f_kept"], "z_before": left["z_side"]},
                {"y_before": right["y_kept"], "f_before": right["f_kept"]},
            ]
        line = right.get("line", line)
        if not step.last:
            g[colour] = right["out"]
            tp, fp, zp, lowp, highp = (
                right[k] for k in ("tp", "fp", "zp", "lowp", "highp")
            )
    count = 1
    for axis in AXES:
        count *= lax.axis_size(axis)
    parts = jnp.broadcast_to(line[None], (count, 1, 128))
    parts = lax.all_to_all(parts, AXES, 0, 0, tiled=True).reshape(count // 8, 8, 128)
    out, monitor = call(
        functools.partial(final_kernel, volume),
        [(2,) + FIELD, (2, ITERS)],
        [(2, ITERS), pltpu.SemaphoreType.DMA((3,))],
        [parts, right["out_n"], right["out_f"], begun],
        10**3,
        hbm_outs=(0, 1),
        aliases={3: 0},
    )
    return (out, monitor)


def solution(mesh):
    finer = Mesh(
        mesh.devices.reshape(8, 2, 2, mesh.shape["gz"], mesh.shape["gy"]),
        AXES,
    )
    return jax.shard_map(
        shards,
        mesh=finer,
        in_specs=(P(None, None, None, TA, "gz", "gy"), P(None, None, TA, "gz", "gy")),
        out_specs=(P(None, None, TA, "gz", "gy"), P()),
        check_vma=False,
    )
```

```python
import functools
import types

import jax
import jax.numpy as jnp
from jax import lax
from jax.experimental import pallas as pl
from jax.experimental.pallas import tpu as pltpu
from jax.sharding import Mesh
from jax.sharding import PartitionSpec as P


ITERS = 2
OMEGA = 1.7
GUARD = 1e-12
TA = ("tz", "tx", "tc")
AXES = TA + ("gz", "gy")
F32 = jnp.float32
R3 = range(3)
PAIRS = ((0, 1), (0, 2), (1, 2))
ROWS = (0, 1, 2, 3, 4, 5, 9, 10, 11, 12, 13, 14)
TWO_ROWS, WHOLE, TURN = range(3)


def re(i, j):
    return 3 * i + j


def im(i, j):
    return 9 + 3 * i + j


def half(h):
    return pl.ds(128 * h, 128)


def three_products(left, right, sign):
    out = [[None] * 9 for _ in R3]
    for k in R3:
        lr = [left(i, k, 0) for i in R3]
        li = [left(i, k, 1) for i in R3]
        rr = [right(j, k, 0) for j in R3]
        ri = [right(j, k, 1) for j in R3]
        ls = [x + y for x, y in zip(lr, li)]
        rs = [x + y if sign > 0 else x - y for x, y in zip(rr, ri)]
        for n, (x, y) in enumerate(((lr, rr), (li, ri), (ls, rs))):
            for i in R3:
                for j in R3:
                    term = x[i] * y[j]
                    old = out[n][re(i, j)]
                    out[n][re(i, j)] = term if old is None else old + term
    return out


def times_adjoint(acc, left, right):
    p, q, s = three_products(
        lambda i, k, n: left(9 * n + re(i, k)), lambda j, k, n: right(9 * n + re(j, k)), -1
    )
    out = [x + y for x, y in zip(p, q)] + [z - (x - y) for x, y, z in zip(p, q, s)]
    return [v if a is None else a + v for a, v in zip(acc, out)]


def times(left, right):
    p, q, s = three_products(
        lambda i, k, n: left(9 * n + re(i, k)), lambda j, k, n: right(9 * n + re(k, j)), 1
    )
    return [x - y for x, y in zip(p, q)] + [z - (x + y) for x, y, z in zip(p, q, s)]


def plus_adjoint(acc, mat):
    out = list(acc)
    for i in R3:
        for j in R3:
            out[re(i, j)] = out[re(i, j)] + mat[re(j, i)]
            out[im(i, j)] = out[im(i, j)] - mat[im(j, i)]
    return out


def rotation(a, p, q):
    v0 = a[re(p, p)] + a[re(q, q)]
    v1 = -(a[im(p, q)] + a[im(q, p)])
    v2 = a[re(q, p)] - a[re(p, q)]
    v3 = -(a[im(p, p)] - a[im(q, q)])
    length = jnp.sqrt(v0 * v0 + v1 * v1 + v2 * v2 + v3 * v3)
    s0 = (1.0 - OMEGA) * length + OMEGA * v0
    s1, s2, s3 = OMEGA * v1, OMEGA * v2, OMEGA * v3
    inverse = lax.rsqrt(s0 * s0 + s1 * s1 + s2 * s2 + s3 * s3 + GUARD)
    return s0 * inverse, s1 * inverse, s2 * inverse, s3 * inverse


def rotate(m, quat, p, q):
    q0, q1, q2, q3 = quat
    out = list(m)
    for j in R3:
        ur, ui = m[re(p, j)], m[im(p, j)]
        lr, li = m[re(q, j)], m[im(q, j)]
        out[re(p, j)] = q0 * ur - q3 * ui + q2 * lr - q1 * li
        out[im(p, j)] = q0 * ui + q3 * ur + q2 * li + q1 * lr
        out[re(q, j)] = q0 * lr + q3 * li - q2 * ur - q1 * ui
        out[im(q, j)] = q0 * li - q3 * lr - q2 * ui + q1 * ur
    return out


def relax(g, w):
    a = times(lambda c: g[c], lambda c: w[c])
    turn = []
    for p, q in PAIRS:
        quat = rotation(a, p, q)
        a = rotate(a, quat, p, q)
        g = rotate(g, quat, p, q)
        turn += quat
    return g, a, turn


def turned(mat, turn):
    for k, (p, q) in enumerate(PAIRS):
        mat = rotate(mat, turn[4 * k : 4 * k + 4], p, q)
    return mat


def third_row(rows):
    a = [None] * 18
    for c, v in zip(ROWS, rows):
        a[c] = v
    for j in R3:
        k, m = (j + 1) % 3, (j + 2) % 3
        ur, ui, xr, xi = a[re(0, k)], a[im(0, k)], a[re(1, m)], a[im(1, m)]
        vr, vi, yr, yi = a[re(0, m)], a[im(0, m)], a[re(1, k)], a[im(1, k)]
        a[re(2, j)] = (ur * xr - ui * xi) - (vr * yr - vi * yi)
        a[im(2, j)] = (vr * yi + vi * yr) - (ur * xi + ui * xr)
    return a


def behind(mode, sent, link, before):
    if mode == TURN:
        return turned([before[c] for c in range(18)], [sent(c) for c in range(12)])
    if mode == TWO_ROWS:
        full = third_row([sent(k) for k in range(12)])
        if link is None:
            return full
        return times_adjoint([None] * 18, lambda c: full[c], link)
    if link is None:
        return [sent(c) for c in range(18)]
    return times_adjoint([None] * 18, sent, link)


def measures(a):
    func = a[re(0, 0)] + a[re(1, 1)] + a[re(2, 2)]
    off = None
    for i, j in PAIRS:
        dr = a[re(i, j)] - a[re(j, i)]
        di = a[im(i, j)] + a[im(j, i)]
        term = dr * dr + di * di
        off = term if off is None else off + term
    mean = (a[im(0, 0)] + a[im(1, 1)] + a[im(2, 2)]) / 3.0
    div = 0.5 * off
    for i in R3:
        d = a[im(i, i)] - mean
        div = div + d * d
    return func, div


def unit(c):
    return 1.0 if c in (0, 4, 8) else 0.0


def crossing(links, h, is_unit):
    return lambda c: jnp.where(is_unit, F32(unit(c)), links[3, c, 1, :, half(h)])


def iotas():
    return (
        lax.broadcasted_iota(jnp.int32, (8, 128), 0),
        lax.broadcasted_iota(jnp.int32, (8, 128), 1),
    )


def slices(core):
    return core, 1 - core


def pack_links(core, links, upz, upy):
    _, lane = iotas()
    for c in range(18):
        upz[c] = jnp.full((8, 128), unit(c), F32)
        for k, s in enumerate(slices(core)):
            for h in range(2):
                r = 4 + 2 * k + h
                upz[c, r : r + 1, :] = links[2, c, s, 7:8, half(h)]
        high0 = pltpu.roll(links[1, c, core, :, half(1)], 96, 1)
        high1 = links[1, c, 1 - core, :, half(1)]
        upy[c] = jnp.where(lane < 64, F32(unit(c)), jnp.where(lane < 96, high0, high1))


def pack_rows(c, k, value, h, scr):
    scr[c, 2 * k + h : 2 * k + h + 1, :] = value[0:1, :]
    scr[c, 4 + 2 * k + h : 5 + 2 * k + h, :] = value[7:8, :]


def pack_z(core, g, upz, zp, scr):
    for c in range(18):
        for k, s in enumerate(slices(core)):
            for h in range(2):
                pack_rows(c, k, g[c, s, :, half(h)], h, scr)
    out = times(lambda c: scr[c], lambda c: upz[c])
    for k, c in enumerate(ROWS if zp.shape[0] == 12 else range(18)):
        zp[k] = out[c]


def row_ends(value):
    _, lane = iotas()
    low1 = pltpu.roll(value(1, 0), 32, 1)
    high0 = pltpu.roll(value(0, 1), 96, 1)
    return jnp.where(
        lane < 64,
        jnp.where(lane < 32, value(0, 0), low1),
        jnp.where(lane < 96, high0, value(1, 1)),
    )


def send_rows(ends, lowp, highp):
    _, lane = iotas()
    for k in range(lowp.shape[0]):
        a, b = ends[2 * k], ends[2 * k + 1]
        lowp[k] = jnp.where(lane < 64, a, pltpu.roll(b, 64, 1))
        highp[k] = jnp.where(lane < 64, pltpu.roll(a, 64, 1), b)


def received(message, c):
    tile = message[c // 2]
    return pltpu.roll(tile, 64, 1) if c % 2 else tile


def pack_y(core, g, upy, lowp, highp):
    ends = [
        row_ends(lambda k, h: g[c, slices(core)[k], :, half(h)]) for c in range(18)
    ]
    out = times(lambda c: ends[c], lambda c: upy[c])
    if lowp.shape[0] == 6:
        out = [out[c] for c in ROWS]
    send_rows(out, lowp, highp)


def first_kernel(links_hbm, g_hbm, tp, fp, zp, lowp, highp, upz, upy, scr, links, g, sems):
    right = pl.ds(128, 128)
    copies = [
        (g_hbm.at[1], g),
        (links_hbm.at[1, 3, :, 1], links.at[3, :, 1]),
        (links_hbm.at[1, 2], links.at[2]),
        (links_hbm.at[1, 1, :, :, :, right], links.at[1, :, :, :, right]),
    ]
    copies = [pltpu.make_async_copy(a, b, sems.at[k]) for k, (a, b) in enumerate(copies)]
    for copy in copies:
        copy.start()
    core = lax.axis_index("tc")
    far, near = slices(core)
    for copy in copies[:2]:
        copy.wait()
    for h in range(2):
        face = times(lambda c: g[c, far, :, half(h)], crossing(links, h, core == 0))
        for k, c in enumerate(ROWS):
            fp[k, :, half(h)] = face[c]
        face = times(lambda c: g[c, near, :, half(h)], crossing(links, h, core == 1))
        for c in range(18):
            tp[c, :, half(h)] = face[c]
    for copy in copies[2:]:
        copy.wait()
    pack_links(core, links, upz, upy)
    pack_z(core, g, upz, zp, scr)
    pack_y(core, g, upy, lowp, highp)


def local_kernel(step, links, gp, *refs):
    refs = list(refs)
    w = refs.pop(0)
    colour = step.colour
    if step.number == 0:
        pack_links(lax.axis_index("tc"), links.at[0], *refs)
    if step.last:
        out, sem = refs
        copy = pltpu.make_async_copy(gp, out.at[1 - colour], sem)
        copy.start()
    first = step.number == 0
    own, other = links.at[colour], links.at[1 - colour]
    if first:
        gp = gp.at[1 - colour]
    row, lane = iotas()
    column = lane % 32
    parity = (row + lane // 32) % 2
    for s in range(2):
        stays = parity == (s + colour) % 2
        behind = []
        for h in range(2):
            behind.append(
                times(lambda c: gp[c, s, :, half(h)], lambda c: other[1, c, s, :, half(h)])
            )
        low, high = [], []
        for c in range(18):
            r0 = pltpu.roll(behind[0][c], 32, 1)
            r1 = pltpu.roll(behind[1][c], 32, 1)
            low.append(jnp.where(lane < 32, 0.0, r0))
            high.append(jnp.where(lane < 32, r0, r1))
        for h, mat in ((0, low), (1, high)):
            acc = plus_adjoint([jnp.zeros((8, 128), F32)] * 18, mat)
            for c in range(18):
                w[c, s, :, half(h)] = acc[c]
        for h in range(2):
            acc = [w[c, s, :, half(h)] for c in range(18)]

            def tile(c):
                return gp[c, s, :, half(h)]

            def ahead_x(c):
                v = tile(c)
                moved = jnp.where(column == 31, pltpu.roll(v, 31, 1), pltpu.roll(v, 127, 1))
                return jnp.where(stays, v, moved)

            acc = times_adjoint(acc, lambda c: own[0, c, s, :, half(h)], ahead_x)

            def ahead_y(c):
                a = pltpu.roll(gp[c, s, :, half(1)], 96, 1)
                if h == 0:
                    return jnp.where(lane >= 96, a, pltpu.roll(tile(c), 96, 1))
                return jnp.where(lane >= 96, 0.0, a)

            acc = times_adjoint(acc, lambda c: own[1, c, s, :, half(h)], ahead_y)

            def ahead_z(c):
                return jnp.where(row == 7, 0.0, pltpu.roll(tile(c), 7, 0))

            acc = times_adjoint(acc, lambda c: own[2, c, s, :, half(h)], ahead_z)
            back = times(tile, lambda c: other[0, c, s, :, half(h)])
            shifted = []
            for v in back:
                moved = jnp.where(column == 0, pltpu.roll(v, 97, 1), pltpu.roll(v, 1, 1))
                shifted.append(jnp.where(stays, moved, v))
            acc = plus_adjoint(acc, shifted)
            back = times(tile, lambda c: other[2, c, s, :, half(h)])
            acc = plus_adjoint(acc, [jnp.where(row == 0, 0.0, pltpu.roll(v, 1, 0)) for v in back])
            if s == 0:
                acc = times_adjoint(
                    acc,
                    lambda c: own[3, c, 0, :, half(h)],
                    lambda c: gp[c, 1, :, half(h)],
                )
            else:
                back = times(
                    lambda c: gp[c, 0, :, half(h)], lambda c: other[3, c, 0, :, half(h)]
                )
                acc = plus_adjoint(acc, back)
            for c in range(18):
                w[c, s, :, half(h)] = acc[c]
    if step.last:
        copy.wait()


def half_kernel(step, h, r):
    own = r.links.at[step.colour]
    g = r.g.at[step.colour] if step.first else r.g
    core = lax.axis_index("tc")
    far, near = slices(core)
    row, lane = iotas()
    if h == 0:
        part = behind(
            step.mode,
            lambda c: r.zh[c],
            lambda c: pltpu.roll(r.upz[c], 4, 0),
            r.z_before if step.mode == TURN else None,
        )
        for c in range(18):
            r.z_side[c] = part[c]
        link = None
        edge, shift = lane < 32, 0
    else:
        link = None if step.mode == TURN else (lambda c: pltpu.roll(r.upy[c], 64, 1))
        edge, shift = lane >= 96, 96
    y_side = behind(
        step.mode,
        lambda c: received(r.y, c),
        link,
        r.y_before if step.mode == TURN else None,
    )
    if step.keeps:
        for c in range(18):
            r.y_kept[c] = y_side[c]

    def with_sides(k, s):
        side = []
        for c in range(18):
            n = 2 * k + h
            up = jnp.broadcast_to(r.z_side[c, n : n + 1, :], (8, 128))
            down = jnp.broadcast_to(r.z_side[c, 4 + n : 5 + n, :], (8, 128))
            across = y_side[c]
            if (shift - 32 * k) % 128:
                across = pltpu.roll(across, (shift - 32 * k) % 128, 1)
            across = jnp.where(edge, across, 0.0)
            side.append(jnp.where(row == 7, up, jnp.where(row == 0, down, 0.0)) + across)
        return plus_adjoint([r.w[c, s, :, half(h)] for c in range(18)], side)

    total = None
    for k, s in ((1, near), (0, far)):
        acc = with_sides(k, s)
        if k == 1:
            link = crossing(own, h, core == 1)
            part = behind(
                WHOLE if step.mode == TWO_ROWS else step.mode,
                lambda c: r.th[c, :, half(h)],
                link,
                r.t_before if step.mode == TURN else None,
            )
            if step.keeps:
                for c in range(18):
                    r.t_kept[c] = part[c]
            acc = plus_adjoint(acc, part)
        else:
            link = crossing(own, h, core == 0)
            part = behind(
                step.mode,
                lambda c: r.fh[c, :, half(h)],
                link,
                r.f_before if step.mode == TURN else None,
            )
            if step.keeps:
                for c in range(18):
                    r.f_kept[c] = part[c]
            acc = plus_adjoint(acc, part)
        new, mat, turn = relax([g[c, s, :, half(h)] for c in range(18)], acc)
        to = (r.new_f, r.new_n)[k]
        for c in range(18):
            to[c] = new[c]
        if step.sends == WHOLE:
            face = times(lambda c: new[c], link)
            to = r.face_n if k == 1 else r.face_f
            for c in range(18):
                to[c] = face[c]
        if step.sends == TURN:
            to = (r.turn_f, r.turn_n)[k]
            for c in range(12):
                to[c] = turn[c]
        if step.colour == 1:
            now = measures(mat)
            total = now if total is None else [a + b for a, b in zip(total, now)]
    if h == 0:
        if step.colour == 1:
            r.sums[0] = total[0]
            r.sums[1] = total[1]
        return
    if step.colour == 1:
        total = [total[0] + r.sums0[0], total[1] + r.sums0[1]]
        place = lax.broadcasted_iota(jnp.int32, (1, 128), 1)
        line = r.line_before[...] if step.number > 1 else jnp.zeros((1, 128), F32)
        for k in range(2):
            rows = jnp.sum(total[k], axis=0, keepdims=True)
            value = jnp.sum(rows, axis=1, keepdims=True)
            line = jnp.where(place == ITERS * k + step.number // 2, value, line)
        r.line[...] = line
    for k, s in ((0, far), (1, near)):
        for c in range(18):
            for j, part in ((0, (r.new_f0, r.new_n0)[k]), (1, (r.new_f, r.new_n)[k])):
                if step.last:
                    (r.out_f, r.out_n)[k][c, :, half(j)] = part[c]
                else:
                    r.out[c, s, :, half(j)] = part[c]
    if step.last:
        return
    if step.sends == WHOLE:
        for c in range(18):
            r.tp[c, :, half(0)] = r.face_n0[c]
            r.tp[c, :, half(1)] = r.face_n[c]
            r.fp[c, :, half(0)] = r.face_f0[c]
            r.fp[c, :, half(1)] = r.face_f[c]
        pack_z(core, r.out, r.upz, r.zp, r.pack_scr)
        pack_y(core, r.out, r.upy, r.lowp, r.highp)
        return
    turns = ((r.turn_f0, r.turn_f), (r.turn_n0, r.turn_n))
    for c in range(12):
        for k in range(2):
            for j in range(2):
                pack_rows(c, k, turns[k][j][c], j, r.zp)
                (r.fp, r.tp)[k][c, :, half(j)] = turns[k][j][c]
    ends = [row_ends(lambda k, j: turns[k][j][c]) for c in range(12)]
    send_rows(ends, r.lowp, r.highp)


def final_kernel(volume, parts, gn, gf, begun, out, monitor, scr, sems):
    copies = [
        pltpu.make_async_copy(part, out.at[1, :, s], sems.at[k])
        for k, (part, s) in enumerate(zip((gf, gn), slices(lax.axis_index("tc"))))
    ]
    for copy in copies:
        copy.start()
    total = parts[0]
    for k in range(1, parts.shape[0]):
        total = total + parts[k]
    total = jnp.sum(total, axis=0, keepdims=True)
    both = jnp.concatenate([total, pltpu.roll(total, 128 - ITERS, 1)], axis=0)
    row = lax.broadcasted_iota(jnp.int32, (2, 128), 0)
    both = jnp.where(row == 0, 1.0 - both / (12.0 * volume), both / (volume / 2.0))
    scr[...] = both[:, :ITERS]
    copies.append(pltpu.make_async_copy(scr, monitor, sems.at[2]))
    copies[2].start()
    for copy in copies:
        copy.wait()


def call(body, outs, scratch, args, flops, hbm=False, hbm_outs=(), aliases={}):
    return pl.pallas_call(
        body,
        out_shape=[jax.ShapeDtypeStruct(o, F32) for o in outs],
        in_specs=[
            pl.BlockSpec(memory_space=pltpu.HBM if hbm or k in aliases else pltpu.VMEM)
            for k in range(len(args))
        ],
        out_specs=[
            pl.BlockSpec(memory_space=pltpu.HBM if k in hbm_outs else pltpu.VMEM)
            for k in range(len(outs))
        ],
        scratch_shapes=[s if not isinstance(s, tuple) else pltpu.VMEM(s, F32) for s in scratch],
        compiler_params=pltpu.CompilerParams(vmem_limit_bytes=24 * 2**20),
        cost_estimate=pl.CostEstimate(flops=flops, bytes_accessed=0, transcendentals=0),
        input_output_aliases=aliases,
    )(*args)


def named(body, ins, outs, scratch):
    names = list(ins) + list(outs) + list(scratch)

    def kernel(*refs):
        body(types.SimpleNamespace(**dict(zip(names, refs))))

    results = call(kernel, list(outs.values()), list(scratch.values()), list(ins.values()), 10**7)
    return dict(zip(outs, results))


def swap(value, axis, partner):
    count = lax.axis_size(axis)
    return lax.ppermute(value, axis, [(i, partner(i) % count) for i in range(count)])


def even_odd(i):
    return i ^ 1


def odd_even(i):
    return i + 1 if i % 2 else i - 1


FACE = (18, 8, 256)
SIDE = (18, 8, 128)
FIELD = (18, 2, 8, 256)
FACE_12 = (12, 8, 256)
SIDE_12 = (12, 8, 128)
ROW = (9, 8, 128)
ROW_12 = (6, 8, 128)
SUMS = (2, 8, 128)
SENT = {WHOLE: [FACE, SIDE, ROW, ROW], TURN: [FACE_12, SIDE_12, ROW_12, ROW_12]}


class Step:
    def __init__(self, number):
        self.number = number
        self.colour = number % 2
        self.first = number < 2
        self.last = number == 2 * ITERS - 1
        self.mode = TWO_ROWS if number == 0 else WHOLE if number == 1 else TURN
        self.keeps = number < 2 * ITERS - 2
        self.sends = None if self.last else WHOLE if number == 0 else TURN


def shards(lattice_links, transform):
    volume = 2 * transform.shape[2] * transform.shape[3] * transform.shape[4]
    for axis in AXES:
        volume *= lax.axis_size(axis)
    tp, fp, zp, lowp, highp, *side = call(
        first_kernel,
        [FACE, FACE_12, SIDE_12, ROW_12, ROW_12, SIDE, SIDE],
        [SIDE, (4,) + FIELD, FIELD, pltpu.SemaphoreType.DMA((4,))],
        [pltpu.with_memory_space_constraint(v, pltpu.HBM) for v in (lattice_links, transform)],
        10**7,
        hbm=True,
    )
    links = lattice_links
    g = [transform, transform]
    packed = [None, side]
    kept = [None, None]
    line = None
    for step in map(Step, range(2 * ITERS)):
        colour = step.colour
        fh = swap(fp, TA, odd_even)
        yu = swap(lowp, "gy", lambda i: i - 1)
        yd = swap(highp, "gy", lambda i: i + 1)
        zh = swap(zp, "gz", even_odd)
        th = swap(tp, "tc", even_odd)
        outs, scratch = [FIELD], []
        if step.number == 0:
            outs += [SIDE, SIDE]
        if step.last:
            outs += [(2,) + FIELD]
            scratch = [pltpu.SemaphoreType.DMA(())]
        w, *rest = call(
            functools.partial(local_kernel, step),
            outs,
            scratch,
            [links, g[1 - colour]],
            3 * 10**7,
            hbm_outs=(1,) if step.last else (),
        )
        if step.number == 0:
            packed[0] = rest
        if step.last:
            (begun,) = rest
        base = {"links": links, "g": g[colour], "w": w, "th": th, "fh": fh}
        outs = {"new_f": SIDE, "new_n": SIDE}
        if step.keeps:
            outs |= {"y_kept": SIDE, "f_kept": SIDE, "t_kept": SIDE}
        if step.sends == WHOLE:
            outs |= {"face_f": SIDE, "face_n": SIDE}
        if step.sends == TURN:
            outs |= {"turn_f": SIDE_12, "turn_n": SIDE_12}
        ins = base | {"zh": zh, "y": yd, "upz": packed[colour][0]}
        if step.mode == TURN:
            ins |= kept[colour][0]
        left = named(
            functools.partial(half_kernel, step, 0),
            ins,
            outs | {"z_side": SIDE} | ({"sums": SUMS} if colour == 1 else {}),
            {},
        )
        ins = base | {"z_side": left["z_side"], "y": yu}
        if step.mode == TURN:
            ins |= kept[colour][1]
        if step.mode != TURN or step.sends == WHOLE:
            ins |= {"upy": packed[colour][1]}
        if step.sends == WHOLE:
            ins |= {"upz": packed[colour][0]}
        ins |= {
            name + "0": left[name]
            for name in ("new_f", "new_n", "face_n", "face_f", "turn_f", "turn_n", "sums")
            if name in left
        }
        if colour == 1 and line is not None:
            ins |= {"line_before": line}
        scratch = {k: v for k, v in outs.items() if not k.endswith("_kept")}
        outs = {k: v for k, v in outs.items() if k.endswith("_kept")}
        if step.last:
            outs |= {"out_f": FACE, "out_n": FACE}
        else:
            outs |= {"out": FIELD, "tp": SENT[step.sends][0]}
            outs |= dict(zip(("fp", "zp", "lowp", "highp"), SENT[step.sends]))
        if colour == 1:
            outs |= {"line": (1, 128)}
        if step.sends == WHOLE:
            scratch |= {"pack_scr": SIDE}
        right = named(functools.partial(half_kernel, step, 1), ins, outs, scratch)
        if step.keeps:
            kept[colour] = [
                {name + "_before": part[name + "_kept"] for name in "yft"}
                for part in (left, right)
            ]
            kept[colour][0]["z_before"] = left["z_side"]
        line = right.get("line", line)
        if not step.last:
            g[colour] = right["out"]
            tp, fp, zp, lowp, highp = (
                right[k] for k in ("tp", "fp", "zp", "lowp", "highp")
            )
    count = 1
    for axis in AXES:
        count *= lax.axis_size(axis)
    parts = jnp.broadcast_to(line[None], (count, 1, 128))
    parts = lax.all_to_all(parts, AXES, 0, 0, tiled=True).reshape(count // 8, 8, 128)
    out, monitor = call(
        functools.partial(final_kernel, volume),
        [(2,) + FIELD, (2, ITERS)],
        [(2, ITERS), pltpu.SemaphoreType.DMA((3,))],
        [parts, right["out_n"], right["out_f"], begun],
        10**3,
        hbm_outs=(0, 1),
        aliases={3: 0},
    )
    return (out, monitor)


def solution(mesh):
    finer = Mesh(
        mesh.devices.reshape(8, 2, 2, mesh.shape["gz"], mesh.shape["gy"]),
        AXES,
    )
    return jax.shard_map(
        shards,
        mesh=finer,
        in_specs=(P(None, None, None, TA, "gz", "gy"), P(None, None, TA, "gz", "gy")),
        out_specs=(P(None, None, TA, "gz", "gy"), P()),
        check_vma=False,
    )
```

```python
import functools
import types

import jax
import jax.numpy as jnp
from jax import lax
from jax.experimental import pallas as pl
from jax.experimental.pallas import tpu as pltpu
from jax.sharding import Mesh
from jax.sharding import PartitionSpec as P


ITERS = 2
OMEGA = 1.7
GUARD = 1e-12
TA = ("tz", "tx", "tc")
AXES = TA + ("gz", "gy")
F32 = jnp.float32
R3 = range(3)
PAIRS = ((0, 1), (0, 2), (1, 2))
ROWS = (0, 1, 2, 3, 4, 5, 9, 10, 11, 12, 13, 14)
TWO_ROWS, WHOLE, TURN = range(3)


def re(i, j):
    return 3 * i + j


def im(i, j):
    return 9 + 3 * i + j


def half(h):
    return pl.ds(128 * h, 128)


def three_products(left, right, sign, out=None):
    if out is None:
        out = [[None] * 9 for _ in R3]
    for k in R3:
        lr = [left(i, k, 0) for i in R3]
        li = [left(i, k, 1) for i in R3]
        rr = [right(j, k, 0) for j in R3]
        ri = [right(j, k, 1) for j in R3]
        ls = [x + y for x, y in zip(lr, li)]
        rs = [x + y if sign > 0 else x - y for x, y in zip(rr, ri)]
        for n, (x, y) in enumerate(((lr, rr), (li, ri), (ls, rs))):
            for i in R3:
                for j in R3:
                    term = x[i] * y[j]
                    old = out[n][re(i, j)]
                    out[n][re(i, j)] = term if old is None else old + term
    return out


def times_adjoint(acc, *pairs):
    sums = None
    for left, right in zip(pairs[::2], pairs[1::2]):
        sums = three_products(
            lambda i, k, n: left(9 * n + re(i, k)),
            lambda j, k, n: right(9 * n + re(j, k)),
            -1,
            sums,
        )
    p, q, s = sums
    out = [x + y for x, y in zip(p, q)] + [z - (x - y) for x, y, z in zip(p, q, s)]
    return [v if a is None else a + v for a, v in zip(acc, out)]


def times(left, right):
    p, q, s = three_products(
        lambda i, k, n: left(9 * n + re(i, k)), lambda j, k, n: right(9 * n + re(k, j)), 1
    )
    return [x - y for x, y in zip(p, q)] + [z - (x + y) for x, y, z in zip(p, q, s)]


def plus_adjoint(acc, mat):
    out = list(acc)
    for i in R3:
        for j in R3:
            out[re(i, j)] = out[re(i, j)] + mat[re(j, i)]
            out[im(i, j)] = out[im(i, j)] - mat[im(j, i)]
    return out


def rotation(a, p, q):
    v0 = a[re(p, p)] + a[re(q, q)]
    v1 = -(a[im(p, q)] + a[im(q, p)])
    v2 = a[re(q, p)] - a[re(p, q)]
    v3 = -(a[im(p, p)] - a[im(q, q)])
    length = jnp.sqrt(v0 * v0 + v1 * v1 + v2 * v2 + v3 * v3)
    s0 = (1.0 - OMEGA) * length + OMEGA * v0
    s1, s2, s3 = OMEGA * v1, OMEGA * v2, OMEGA * v3
    inverse = lax.rsqrt(s0 * s0 + s1 * s1 + s2 * s2 + s3 * s3 + GUARD)
    return s0 * inverse, s1 * inverse, s2 * inverse, s3 * inverse


def rotate(m, quat, p, q):
    q0, q1, q2, q3 = quat
    out = list(m)
    for j in R3:
        ur, ui = m[re(p, j)], m[im(p, j)]
        lr, li = m[re(q, j)], m[im(q, j)]
        out[re(p, j)] = q0 * ur - q3 * ui + q2 * lr - q1 * li
        out[im(p, j)] = q0 * ui + q3 * ur + q2 * li + q1 * lr
        out[re(q, j)] = q0 * lr + q3 * li - q2 * ur - q1 * ui
        out[im(q, j)] = q0 * li - q3 * lr - q2 * ui + q1 * ur
    return out


def relax(g, w):
    a = times(lambda c: g[c], lambda c: w[c])
    turn = []
    for p, q in PAIRS:
        quat = rotation(a, p, q)
        a = rotate(a, quat, p, q)
        g = rotate(g, quat, p, q)
        turn += quat
    return g, a, turn


def turned(mat, turn):
    for k, (p, q) in enumerate(PAIRS):
        mat = rotate(mat, turn[4 * k : 4 * k + 4], p, q)
    return mat


def third_row(rows):
    a = [None] * 18
    for c, v in zip(ROWS, rows):
        a[c] = v
    for j in R3:
        k, m = (j + 1) % 3, (j + 2) % 3
        ur, ui, xr, xi = a[re(0, k)], a[im(0, k)], a[re(1, m)], a[im(1, m)]
        vr, vi, yr, yi = a[re(0, m)], a[im(0, m)], a[re(1, k)], a[im(1, k)]
        a[re(2, j)] = (ur * xr - ui * xi) - (vr * yr - vi * yi)
        a[im(2, j)] = (vr * yi + vi * yr) - (ur * xi + ui * xr)
    return a


def behind(mode, sent, link, before):
    if mode == TURN:
        return turned([before[c] for c in range(18)], [sent(c) for c in range(12)])
    if mode == TWO_ROWS:
        full = third_row([sent(k) for k in range(12)])
        if link is None:
            return full
        return times_adjoint([None] * 18, lambda c: full[c], link)
    if link is None:
        return [sent(c) for c in range(18)]
    return times_adjoint([None] * 18, sent, link)


def measures(a):
    func = a[re(0, 0)] + a[re(1, 1)] + a[re(2, 2)]
    off = None
    for i, j in PAIRS:
        dr = a[re(i, j)] - a[re(j, i)]
        di = a[im(i, j)] + a[im(j, i)]
        term = dr * dr + di * di
        off = term if off is None else off + term
    mean = (a[im(0, 0)] + a[im(1, 1)] + a[im(2, 2)]) / 3.0
    div = 0.5 * off
    for i in R3:
        d = a[im(i, i)] - mean
        div = div + d * d
    return func, div


def unit(c):
    return 1.0 if c in (0, 4, 8) else 0.0


def crossing(links, h, is_unit):
    return lambda c: jnp.where(is_unit, F32(unit(c)), links[3, c, 1, :, half(h)])


def iotas():
    return (
        lax.broadcasted_iota(jnp.int32, (8, 128), 0),
        lax.broadcasted_iota(jnp.int32, (8, 128), 1),
    )


def slices(core):
    return core, 1 - core


def pack_links(core, links, upz, upy):
    _, lane = iotas()
    for c in range(18):
        upz[c] = jnp.full((8, 128), unit(c), F32)
        for k, s in enumerate(slices(core)):
            for h in range(2):
                r = 4 + 2 * k + h
                upz[c, r : r + 1, :] = links[2, c, s, 7:8, half(h)]
        high0 = pltpu.roll(links[1, c, core, :, half(1)], 96, 1)
        high1 = links[1, c, 1 - core, :, half(1)]
        upy[c] = jnp.where(lane < 64, F32(unit(c)), jnp.where(lane < 96, high0, high1))


def pack_rows(c, k, value, h, scr):
    scr[c, 2 * k + h : 2 * k + h + 1, :] = value[0:1, :]
    scr[c, 4 + 2 * k + h : 5 + 2 * k + h, :] = value[7:8, :]


def pack_z(core, g, upz, zp, scr):
    for c in range(18):
        for k, s in enumerate(slices(core)):
            for h in range(2):
                pack_rows(c, k, g[c, s, :, half(h)], h, scr)
    out = times(lambda c: scr[c], lambda c: upz[c])
    for k, c in enumerate(ROWS if zp.shape[0] == 12 else range(18)):
        zp[k] = out[c]


def row_ends(value):
    _, lane = iotas()
    low1 = pltpu.roll(value(1, 0), 32, 1)
    high0 = pltpu.roll(value(0, 1), 96, 1)
    return jnp.where(
        lane < 64,
        jnp.where(lane < 32, value(0, 0), low1),
        jnp.where(lane < 96, high0, value(1, 1)),
    )


def send_rows(ends, lowp, highp):
    _, lane = iotas()
    for k in range(lowp.shape[0]):
        a, b = ends[2 * k], ends[2 * k + 1]
        lowp[k] = jnp.where(lane < 64, a, pltpu.roll(b, 64, 1))
        highp[k] = jnp.where(lane < 64, pltpu.roll(a, 64, 1), b)


def received(message, c):
    tile = message[c // 2]
    return pltpu.roll(tile, 64, 1) if c % 2 else tile


def pack_y(core, g, upy, lowp, highp):
    ends = [
        row_ends(lambda k, h: g[c, slices(core)[k], :, half(h)]) for c in range(18)
    ]
    out = times(lambda c: ends[c], lambda c: upy[c])
    if lowp.shape[0] == 6:
        out = [out[c] for c in ROWS]
    send_rows(out, lowp, highp)


def first_kernel(links_hbm, g_hbm, tp, fp, zp, lowp, highp, upz, upy, scr, links, g, sems):
    right = pl.ds(128, 128)
    copies = [
        (g_hbm.at[1], g),
        (links_hbm.at[1, 3, :, 1], links.at[3, :, 1]),
        (links_hbm.at[1, 2], links.at[2]),
        (links_hbm.at[1, 1, :, :, :, right], links.at[1, :, :, :, right]),
    ]
    copies = [pltpu.make_async_copy(a, b, sems.at[k]) for k, (a, b) in enumerate(copies)]
    for copy in copies:
        copy.start()
    core = lax.axis_index("tc")
    far, near = slices(core)
    for copy in copies[:2]:
        copy.wait()
    for h in range(2):
        face = times(lambda c: g[c, far, :, half(h)], crossing(links, h, core == 0))
        for k, c in enumerate(ROWS):
            fp[k, :, half(h)] = face[c]
        face = times(lambda c: g[c, near, :, half(h)], crossing(links, h, core == 1))
        for c in range(18):
            tp[c, :, half(h)] = face[c]
    for copy in copies[2:]:
        copy.wait()
    pack_links(core, links, upz, upy)
    pack_z(core, g, upz, zp, scr)
    pack_y(core, g, upy, lowp, highp)


def local_kernel(step, links, gp, *refs):
    refs = list(refs)
    w = refs.pop(0)
    colour = step.colour
    if step.number == 0:
        pack_links(lax.axis_index("tc"), links.at[0], *refs)
    if step.last:
        out, sem = refs
        copy = pltpu.make_async_copy(gp, out.at[1 - colour], sem)
        copy.start()
    first = step.number == 0
    own, other = links.at[colour], links.at[1 - colour]
    if first:
        gp = gp.at[1 - colour]
    row, lane = iotas()
    column = lane % 32
    parity = (row + lane // 32) % 2
    for s in range(2):
        stays = parity == (s + colour) % 2
        behind = []
        for h in range(2):
            behind.append(
                times(lambda c: gp[c, s, :, half(h)], lambda c: other[1, c, s, :, half(h)])
            )
        low, high = [], []
        for c in range(18):
            r0 = pltpu.roll(behind[0][c], 32, 1)
            r1 = pltpu.roll(behind[1][c], 32, 1)
            low.append(jnp.where(lane < 32, 0.0, r0))
            high.append(jnp.where(lane < 32, r0, r1))
        for h, mat in ((0, low), (1, high)):
            acc = plus_adjoint([jnp.zeros((8, 128), F32)] * 18, mat)
            for c in range(18):
                w[c, s, :, half(h)] = acc[c]
        for h in range(2):
            acc = [w[c, s, :, half(h)] for c in range(18)]

            def tile(c):
                return gp[c, s, :, half(h)]

            def ahead_x(c):
                v = tile(c)
                moved = jnp.where(column == 31, pltpu.roll(v, 31, 1), pltpu.roll(v, 127, 1))
                return jnp.where(stays, v, moved)


            def ahead_y(c):
                a = pltpu.roll(gp[c, s, :, half(1)], 96, 1)
                if h == 0:
                    return jnp.where(lane >= 96, a, pltpu.roll(tile(c), 96, 1))
                return jnp.where(lane >= 96, 0.0, a)


            def ahead_z(c):
                return jnp.where(row == 7, 0.0, pltpu.roll(tile(c), 7, 0))

            ahead = []
            for mu, value in enumerate((ahead_x, ahead_y, ahead_z)):
                ahead += [lambda c, mu=mu: own[mu, c, s, :, half(h)], value]
            if s == 0:
                ahead += [lambda c: own[3, c, 0, :, half(h)], lambda c: gp[c, 1, :, half(h)]]
            acc = times_adjoint(acc, *ahead)
            back = times(tile, lambda c: other[0, c, s, :, half(h)])
            shifted = []
            for v in back:
                moved = jnp.where(column == 0, pltpu.roll(v, 97, 1), pltpu.roll(v, 1, 1))
                shifted.append(jnp.where(stays, moved, v))
            acc = plus_adjoint(acc, shifted)
            back = times(tile, lambda c: other[2, c, s, :, half(h)])
            acc = plus_adjoint(acc, [jnp.where(row == 0, 0.0, pltpu.roll(v, 1, 0)) for v in back])
            if s == 1:
                back = times(
                    lambda c: gp[c, 0, :, half(h)], lambda c: other[3, c, 0, :, half(h)]
                )
                acc = plus_adjoint(acc, back)
            for c in range(18):
                w[c, s, :, half(h)] = acc[c]
    if step.last:
        copy.wait()


def half_kernel(step, h, r):
    own = r.links.at[step.colour]
    g = r.g.at[step.colour] if step.first else r.g
    core = lax.axis_index("tc")
    far, near = slices(core)
    row, lane = iotas()
    if h == 0:
        part = behind(
            step.mode,
            lambda c: r.zh[c],
            lambda c: pltpu.roll(r.upz[c], 4, 0),
            r.z_before if step.mode == TURN else None,
        )
        for c in range(18):
            r.z_side[c] = part[c]
        link = None
        edge, shift = lane < 32, 0
    else:
        link = None if step.mode == TURN else (lambda c: pltpu.roll(r.upy[c], 64, 1))
        edge, shift = lane >= 96, 96
    y_side = behind(
        step.mode,
        lambda c: received(r.y, c),
        link,
        r.y_before if step.mode == TURN else None,
    )
    if step.keeps:
        for c in range(18):
            r.y_kept[c] = y_side[c]

    def with_sides(k, s):
        side = []
        for c in range(18):
            n = 2 * k + h
            up = jnp.broadcast_to(r.z_side[c, n : n + 1, :], (8, 128))
            down = jnp.broadcast_to(r.z_side[c, 4 + n : 5 + n, :], (8, 128))
            across = y_side[c]
            if (shift - 32 * k) % 128:
                across = pltpu.roll(across, (shift - 32 * k) % 128, 1)
            across = jnp.where(edge, across, 0.0)
            side.append(jnp.where(row == 7, up, jnp.where(row == 0, down, 0.0)) + across)
        return plus_adjoint([r.w[c, s, :, half(h)] for c in range(18)], side)

    total = None
    for k, s in ((1, near), (0, far)):
        acc = with_sides(k, s)
        if k == 1:
            link = crossing(own, h, core == 1)
            part = behind(
                WHOLE if step.mode == TWO_ROWS else step.mode,
                lambda c: r.th[c, :, half(h)],
                link,
                r.t_before if step.mode == TURN else None,
            )
            if step.keeps:
                for c in range(18):
                    r.t_kept[c] = part[c]
            acc = plus_adjoint(acc, part)
        else:
            link = crossing(own, h, core == 0)
            part = behind(
                step.mode,
                lambda c: r.fh[c, :, half(h)],
                link,
                r.f_before if step.mode == TURN else None,
            )
            if step.keeps:
                for c in range(18):
                    r.f_kept[c] = part[c]
            acc = plus_adjoint(acc, part)
        new, mat, turn = relax([g[c, s, :, half(h)] for c in range(18)], acc)
        to = (r.new_f, r.new_n)[k]
        for c in range(18):
            to[c] = new[c]
        if step.sends == WHOLE:
            face = times(lambda c: new[c], link)
            to = r.face_n if k == 1 else r.face_f
            for c in range(18):
                to[c] = face[c]
        if step.sends == TURN:
            to = (r.turn_f, r.turn_n)[k]
            for c in range(12):
                to[c] = turn[c]
        if step.colour == 1:
            now = measures(mat)
            total = now if total is None else [a + b for a, b in zip(total, now)]
    if h == 0:
        if step.colour == 1:
            r.sums[0] = total[0]
            r.sums[1] = total[1]
        return
    if step.colour == 1:
        total = [total[0] + r.sums0[0], total[1] + r.sums0[1]]
        place = lax.broadcasted_iota(jnp.int32, (1, 128), 1)
        line = r.line_before[...] if step.number > 1 else jnp.zeros((1, 128), F32)
        for k in range(2):
            rows = jnp.sum(total[k], axis=0, keepdims=True)
            value = jnp.sum(rows, axis=1, keepdims=True)
            line = jnp.where(place == ITERS * k + step.number // 2, value, line)
        r.line[...] = line
    for k, s in ((0, far), (1, near)):
        for c in range(18):
            for j, part in ((0, (r.new_f0, r.new_n0)[k]), (1, (r.new_f, r.new_n)[k])):
                if step.last:
                    (r.out_f, r.out_n)[k][c, :, half(j)] = part[c]
                else:
                    r.out[c, s, :, half(j)] = part[c]
    if step.last:
        return
    if step.sends == WHOLE:
        for c in range(18):
            r.tp[c, :, half(0)] = r.face_n0[c]
            r.tp[c, :, half(1)] = r.face_n[c]
            r.fp[c, :, half(0)] = r.face_f0[c]
            r.fp[c, :, half(1)] = r.face_f[c]
        pack_z(core, r.out, r.upz, r.zp, r.pack_scr)
        pack_y(core, r.out, r.upy, r.lowp, r.highp)
        return
    turns = ((r.turn_f0, r.turn_f), (r.turn_n0, r.turn_n))
    for c in range(12):
        for k in range(2):
            for j in range(2):
                pack_rows(c, k, turns[k][j][c], j, r.zp)
                (r.fp, r.tp)[k][c, :, half(j)] = turns[k][j][c]
    ends = [row_ends(lambda k, j: turns[k][j][c]) for c in range(12)]
    send_rows(ends, r.lowp, r.highp)


def final_kernel(volume, parts, gn, gf, begun, out, monitor, scr, sems):
    copies = [
        pltpu.make_async_copy(part, out.at[1, :, s], sems.at[k])
        for k, (part, s) in enumerate(zip((gf, gn), slices(lax.axis_index("tc"))))
    ]
    for copy in copies:
        copy.start()
    total = parts[0]
    for k in range(1, parts.shape[0]):
        total = total + parts[k]
    total = jnp.sum(total, axis=0, keepdims=True)
    both = jnp.concatenate([total, pltpu.roll(total, 128 - ITERS, 1)], axis=0)
    row = lax.broadcasted_iota(jnp.int32, (2, 128), 0)
    both = jnp.where(row == 0, 1.0 - both / (12.0 * volume), both / (volume / 2.0))
    scr[...] = both[:, :ITERS]
    copies.append(pltpu.make_async_copy(scr, monitor, sems.at[2]))
    copies[2].start()
    for copy in copies:
        copy.wait()


def call(body, outs, scratch, args, flops, hbm=False, hbm_outs=(), aliases={}):
    return pl.pallas_call(
        body,
        out_shape=[jax.ShapeDtypeStruct(o, F32) for o in outs],
        in_specs=[
            pl.BlockSpec(memory_space=pltpu.HBM if hbm or k in aliases else pltpu.VMEM)
            for k in range(len(args))
        ],
        out_specs=[
            pl.BlockSpec(memory_space=pltpu.HBM if k in hbm_outs else pltpu.VMEM)
            for k in range(len(outs))
        ],
        scratch_shapes=[s if not isinstance(s, tuple) else pltpu.VMEM(s, F32) for s in scratch],
        compiler_params=pltpu.CompilerParams(vmem_limit_bytes=24 * 2**20),
        cost_estimate=pl.CostEstimate(flops=flops, bytes_accessed=0, transcendentals=0),
        input_output_aliases=aliases,
    )(*args)


def named(body, ins, outs, scratch):
    names = list(ins) + list(outs) + list(scratch)

    def kernel(*refs):
        body(types.SimpleNamespace(**dict(zip(names, refs))))

    results = call(kernel, list(outs.values()), list(scratch.values()), list(ins.values()), 10**7)
    return dict(zip(outs, results))


def swap(value, axis, partner):
    count = lax.axis_size(axis)
    return lax.ppermute(value, axis, [(i, partner(i) % count) for i in range(count)])


def even_odd(i):
    return i ^ 1


def odd_even(i):
    return i + 1 if i % 2 else i - 1


FACE = (18, 8, 256)
SIDE = (18, 8, 128)
FIELD = (18, 2, 8, 256)
FACE_12 = (12, 8, 256)
SIDE_12 = (12, 8, 128)
ROW = (9, 8, 128)
ROW_12 = (6, 8, 128)
SUMS = (2, 8, 128)
SENT = {WHOLE: [FACE, SIDE, ROW, ROW], TURN: [FACE_12, SIDE_12, ROW_12, ROW_12]}


class Step:
    def __init__(self, number):
        self.number = number
        self.colour = number % 2
        self.first = number < 2
        self.last = number == 2 * ITERS - 1
        self.mode = TWO_ROWS if number == 0 else WHOLE if number == 1 else TURN
        self.keeps = number < 2 * ITERS - 2
        self.sends = None if self.last else WHOLE if number == 0 else TURN


def shards(lattice_links, transform):
    volume = 2 * transform.shape[2] * transform.shape[3] * transform.shape[4]
    for axis in AXES:
        volume *= lax.axis_size(axis)
    tp, fp, zp, lowp, highp, *side = call(
        first_kernel,
        [FACE, FACE_12, SIDE_12, ROW_12, ROW_12, SIDE, SIDE],
        [SIDE, (4,) + FIELD, FIELD, pltpu.SemaphoreType.DMA((4,))],
        [pltpu.with_memory_space_constraint(v, pltpu.HBM) for v in (lattice_links, transform)],
        10**7,
        hbm=True,
    )
    links = lattice_links
    g = [transform, transform]
    packed = [None, side]
    kept = [None, None]
    line = None
    for step in map(Step, range(2 * ITERS)):
        colour = step.colour
        fh = swap(fp, TA, odd_even)
        yu = swap(lowp, "gy", lambda i: i - 1)
        yd = swap(highp, "gy", lambda i: i + 1)
        zh = swap(zp, "gz", even_odd)
        th = swap(tp, "tc", even_odd)
        outs, scratch = [FIELD], []
        if step.number == 0:
            outs += [SIDE, SIDE]
        if step.last:
            outs += [(2,) + FIELD]
            scratch = [pltpu.SemaphoreType.DMA(())]
        w, *rest = call(
            functools.partial(local_kernel, step),
            outs,
            scratch,
            [links, g[1 - colour]],
            3 * 10**7,
            hbm_outs=(1,) if step.last else (),
        )
        if step.number == 0:
            packed[0] = rest
        if step.last:
            (begun,) = rest
        base = {"links": links, "g": g[colour], "w": w, "th": th, "fh": fh}
        outs = {"new_f": SIDE, "new_n": SIDE}
        if step.keeps:
            outs |= {"y_kept": SIDE, "f_kept": SIDE, "t_kept": SIDE}
        if step.sends == WHOLE:
            outs |= {"face_f": SIDE, "face_n": SIDE}
        if step.sends == TURN:
            outs |= {"turn_f": SIDE_12, "turn_n": SIDE_12}
        ins = base | {"zh": zh, "y": yd, "upz": packed[colour][0]}
        if step.mode == TURN:
            ins |= kept[colour][0]
        left = named(
            functools.partial(half_kernel, step, 0),
            ins,
            outs | {"z_side": SIDE} | ({"sums": SUMS} if colour == 1 else {}),
            {},
        )
        ins = base | {"z_side": left["z_side"], "y": yu}
        if step.mode == TURN:
            ins |= kept[colour][1]
        if step.mode != TURN or step.sends == WHOLE:
            ins |= {"upy": packed[colour][1]}
        if step.sends == WHOLE:
            ins |= {"upz": packed[colour][0]}
        ins |= {
            name + "0": left[name]
            for name in ("new_f", "new_n", "face_n", "face_f", "turn_f", "turn_n", "sums")
            if name in left
        }
        if colour == 1 and line is not None:
            ins |= {"line_before": line}
        scratch = {k: v for k, v in outs.items() if not k.endswith("_kept")}
        outs = {k: v for k, v in outs.items() if k.endswith("_kept")}
        if step.last:
            outs |= {"out_f": FACE, "out_n": FACE}
        else:
            outs |= {"out": FIELD, "tp": SENT[step.sends][0]}
            outs |= dict(zip(("fp", "zp", "lowp", "highp"), SENT[step.sends]))
        if colour == 1:
            outs |= {"line": (1, 128)}
        if step.sends == WHOLE:
            scratch |= {"pack_scr": SIDE}
        right = named(functools.partial(half_kernel, step, 1), ins, outs, scratch)
        if step.keeps:
            kept[colour] = [
                {name + "_before": part[name + "_kept"] for name in "yft"}
                for part in (left, right)
            ]
            kept[colour][0]["z_before"] = left["z_side"]
        line = right.get("line", line)
        if not step.last:
            g[colour] = right["out"]
            tp, fp, zp, lowp, highp = (
                right[k] for k in ("tp", "fp", "zp", "lowp", "highp")
            )
    count = 1
    for axis in AXES:
        count *= lax.axis_size(axis)
    parts = jnp.broadcast_to(line[None], (count, 1, 128))
    parts = lax.all_to_all(parts, AXES, 0, 0, tiled=True).reshape(count // 8, 8, 128)
    out, monitor = call(
        functools.partial(final_kernel, volume),
        [(2,) + FIELD, (2, ITERS)],
        [(2, ITERS), pltpu.SemaphoreType.DMA((3,))],
        [parts, right["out_n"], right["out_f"], begun],
        10**3,
        hbm_outs=(0, 1),
        aliases={3: 0},
    )
    return (out, monitor)


def solution(mesh):
    finer = Mesh(
        mesh.devices.reshape(8, 2, 2, mesh.shape["gz"], mesh.shape["gy"]),
        AXES,
    )
    return jax.shard_map(
        shards,
        mesh=finer,
        in_specs=(P(None, None, None, TA, "gz", "gy"), P(None, None, TA, "gz", "gy")),
        out_specs=(P(None, None, TA, "gz", "gy"), P()),
        check_vma=False,
    )
```
